256 devices in a mesh: parts: 2 (over y), row: 128 (over z, x, core).
Axes of the slice: x: 4, y: 2, z: 16, core: 2. Of those that a mesh axis runs over, the one named last changes fastest.
The devices are a block of a 4x16x16 slice.
Arguments:
- tokens: bfloat16 [512, 256, 768], P(('parts', 'row')), parts along dimension 0, may hold values from -6 to 6
- w_query: bfloat16 [768, 768], replicated, may hold values from -0.21875 to 0.21875
- w_key: bfloat16 [768, 768], replicated, may hold values from -0.21875 to 0.21875
- w_value: bfloat16 [768, 768], replicated, may hold values from -0.21875 to 0.21875
- w_out: bfloat16 [768, 768], replicated, may hold values from -0.21875 to 0.21875
- omega: bfloat16 [12, 64, 256], replicated, may hold values from -5 to 5
- conv_kernel: float32 [3, 3, 768], replicated, may hold values from -0.6 to 0.6
- norm_gain: float32 [768], replicated, may hold values from 0.1 to 1.9
Outputs:
- layer_out: bfloat16 [512, 256, 768], P(('parts', 'row')), parts along dimension 0
The draws below stay inside these ranges and needn't reach their ends.
There are 2 independent parts, one for each index of `parts`. The reference program is written for one: setup_inputs(seed, part) draws one part's arguments, and reference() takes and returns one part's arrays. A program takes and returns all parts, laid end to end along the dimension named above; an argument that names none is the same for every part. Nothing has to cross between parts.
All inputs are finite; a program needn't handle non-finite values.
Results may differ from the reference program's by a relative error of at most 0.0081.
Values may be sent and summed in bfloat16 or wider, within the bound.
A program may use at most 64 MiB of HBM per device.

```python
import jax
import jax.numpy as jnp
from jax import lax

D = 768
HEADS = 12
DH = 64
FEAT = 256
COLS = 256
ROWS_DEV = 2
GRID_ROWS = 256


def block_scale(stream_key, shape, split, low, high):
    def one(dim, shards_of):
        heights = jax.random.uniform(jax.random.fold_in(jax.random.fold_in(stream_key, 6), dim), (shards_of,), jnp.float32, low / len(split), high / len(split))
        return jnp.repeat(jnp.exp(heights), shape[dim] // shards_of).reshape((-1,) + (1,) * (len(shape) - dim - 1))

    factor_of = one(*split[0])
    for cut in split[1:]:
        factor_of = factor_of * one(*cut)
    return factor_of


def centred(stream_key, dims, scale, bound, shards=(), held_as=jnp.bfloat16):
    gain = block_scale(stream_key, dims, shards, -0.22, 0.18) if shards else 1.0
    values = jax.random.normal(stream_key, dims, jnp.float32) * scale * gain
    return jnp.minimum(jnp.maximum(values, -bound), bound).astype(held_as)


def setup_inputs(seed: int = 0, part: int = 0) -> dict:
    streams_of = jax.random.split(jax.random.key(seed), 9)
    own_keys = jax.random.split(jax.random.fold_in(streams_of[8], part), 9)
    tokens = centred(own_keys[0], (GRID_ROWS, COLS, D), 1.0, 6.0, ((0, 128),))
    w_query = centred(streams_of[1], (D, D), D ** -0.5, 0.21875)
    w_key = centred(streams_of[2], (D, D), D ** -0.5, 0.21875)
    w_value = centred(streams_of[3], (D, D), D ** -0.5, 0.21875)
    w_out = centred(streams_of[4], (D, D), D ** -0.5, 0.21875)
    omega = centred(streams_of[5], (HEADS, DH, FEAT), 1.0, 5.0)
    conv_kernel = jnp.clip(jax.random.uniform(streams_of[6], (3, 3, D), jnp.float32, -0.6, 0.6), -0.6, 0.6)
    norm_gain = jnp.clip(1.0 + 0.18 * jax.random.normal(streams_of[7], (D,), jnp.float32), 0.1, 1.9)
    return {"tokens": tokens, "w_query": w_query, "w_key": w_key, "w_value": w_value, "w_out": w_out, "omega": omega, "conv_kernel": conv_kernel, "norm_gain": norm_gain}


def project(rows, weight):
    return jnp.dot(rows, weight, preferred_element_type=jnp.float32).astype(jnp.bfloat16)

def feature_map(heads_in, omega):
    dim_head = heads_in.shape[-1]
    values = heads_in.astype(jnp.float32)
    lifted = jnp.einsum('thd,hdf->thf', values, omega.astype(jnp.float32))
    square = lax.optimization_barrier(jnp.sum(values * values, axis=-1, keepdims=True))
    feats = jnp.exp(lifted * dim_head ** (-0.25) - square * 0.5 * dim_head ** (-0.5)) * omega.shape[-1] ** (-0.5)
    return feats.astype(jnp.bfloat16)

def reference(tokens, w_query, w_key, w_value, w_out, omega, conv_kernel, norm_gain):
    grid_rows, cols, width = tokens.shape
    heads, dim_head, nfeat = omega.shape
    blocks = grid_rows // ROWS_DEV
    flat = tokens.reshape(grid_rows * cols, width)
    value = project(flat, w_value)
    value_blocks = value.reshape(blocks, ROWS_DEV * cols, heads, dim_head)
    token_blocks = tokens.reshape(blocks, ROWS_DEV * cols, width)

    def add_state(carry, pair):
        rows, vals = pair
        feat_key = feature_map(project(rows, w_key).reshape(-1, heads, dim_head), omega).astype(jnp.float32)
        state = carry[0] + jnp.einsum('thf,thd->fhd', feat_key, vals.astype(jnp.float32))
        total = carry[1] + lax.optimization_barrier(jnp.sum(feat_key, axis=0)).astype(jnp.float32)
        return ((state, total), None)
    init = (jnp.zeros((nfeat, heads, dim_head), jnp.float32), jnp.zeros((heads, nfeat), jnp.float32))
    (kv_sum, key_sum), unused = lax.scan(add_state, init, (token_blocks, value_blocks))
    kv_state = kv_sum.astype(jnp.bfloat16).astype(jnp.float32)
    padded = jnp.pad(value.reshape(grid_rows, cols, width).astype(jnp.float32), ((1, 1), (1, 1), (0, 0)))
    position = jnp.zeros((grid_rows, cols, width), jnp.float32)
    for shift_a in range(3):
        for shift_b in range(3):
            position = position + padded[shift_a:shift_a + grid_rows, shift_b:shift_b + cols, :] * conv_kernel[shift_a, shift_b]
    position_blocks = position.reshape(blocks, ROWS_DEV * cols, width)

    def block_out(pair):
        rows, local_pos = pair
        feat_query = feature_map(project(rows, w_query).reshape(-1, heads, dim_head), omega).astype(jnp.float32)
        numer = jnp.einsum('thf,fhd->thd', feat_query, kv_state, precision=lax.Precision.HIGHEST)
        denom = jnp.einsum('thf,hf->th', feat_query, key_sum, precision=lax.Precision.HIGHEST)
        attn = numer / denom[:, :, None]
        scale = lax.rsqrt(lax.optimization_barrier(jnp.mean(attn * attn, axis=(1, 2), keepdims=True)) + 1e-06)
        normed = (attn * scale).reshape(-1, width) * norm_gain
        mixed = (normed + local_pos).astype(jnp.bfloat16)
        out = rows.astype(jnp.float32) + jnp.dot(mixed, w_out, preferred_element_type=jnp.float32)
        return out.astype(jnp.bfloat16)
    outs = lax.map(block_out, (token_blocks, position_blocks))
    return outs.reshape(grid_rows, cols, width)
```

```python
import functools
import math

import jax
import jax.numpy as jnp
from jax import lax
from jax.experimental import pallas as pl
from jax.experimental.pallas import tpu as pltpu
from jax.sharding import PartitionSpec as P

MESH = pl.DeviceIdType.MESH
F32 = jnp.float32
BF16 = jnp.bfloat16

XS = 4
ZN = 4
CORES = 2
NEAR = XS * ZN
KV_ROWS = 48
CHUNK = 64


def near_peer(zl, x, a, b):
    if a == 0:
        zp = zl
    elif a == 1:
        zp = zl + 1 - 2 * (zl % 2)
    elif a == 2:
        zp = (zl + 2) % 4
    else:
        zp = 3 - zl
    return zp * XS + (x + b) % XS


STEPS = [(a, b) for a in (3, 2, 1) for b in (2, 1, 3, 0)] + [(0, b) for b in (2, 1, 3)]


def back_step(b):
    return (XS - b) % XS


def dot(a, b):
    return jnp.dot(a, b, preferred_element_type=F32)


def dot_t(a, b):
    return lax.dot_general(a, b, (((1,), (1,)), ((), ())), preferred_element_type=F32)


def features(u, omega_pad, kappa, lift, dim_head):
    nfeat = omega_pad[0].shape[-1]
    u32 = u.astype(F32)
    square = u32 * u32 * (-lift) - (0.5 * math.log2(nfeat) / kappa / dim_head)
    high = square.astype(BF16).astype(F32)
    low = pltpu.roll(square - high, dim_head, 1)
    first = lax.broadcasted_iota(jnp.int32, square.shape, 1) < dim_head
    out = []
    for s in range(2):
        parts = jnp.where(first, high, low) if s == 0 else jnp.where(first, low, high)
        lhs = jnp.concatenate([u, parts.astype(BF16)], axis=1)
        arg = dot(lhs, omega_pad[s])
        out.append(jnp.exp2(arg * kappa).astype(BF16))
    return out


def kernel(
    n,
    heads,
    tok_h,
    wq_h,
    wk_h,
    wv_h,
    wo_h,
    om_h,
    ck_h,
    gain_h,
    out_h,
    tok,
    wq,
    wk,
    wv,
    wo,
    om,
    ck,
    gain,
    omp,
    proj,
    vext,
    halo,
    vt,
    fq,
    pos,
    attn,
    mixed,
    outv,
    send0,
    recv0,
    send1,
    recv1,
    send2,
    recv2,
    state,
    rhs,
    in_sem,
    out_sem,
    pair_sem,
    halo_sem,
    rs_sem,
    far_sem,
    ag_sem,
    fw_sem,
):
    tokens, width = tok.shape
    cols = halo.shape[1]
    rows_here = tokens // cols
    dim_head = width // heads
    nfeat = om.shape[-1]
    pairs = heads // 2
    lanes = 2 * dim_head
    half = nfeat // 2
    kappa = dim_head ** (-0.25) * math.log2(math.e)
    lift = 0.5 * dim_head ** (-0.5) / dim_head ** (-0.25)

    me = lax.axis_index("row")
    core = me % CORES
    near = (me // CORES) % NEAR
    zl, x = near // XS, near % XS
    far_count = n // (CORES * NEAR)
    far = me // (CORES * NEAR)
    base = far * (CORES * NEAR) + core

    partner = me + 1 - 2 * core
    above, below = (me + n - 1) % n, (me + 1) % n
    near_ids = [(s, near_peer(zl, x, *s)) for s in STEPS]
    far_ids = [
        ((far + d) % far_count) * (CORES * NEAR) + near * CORES + core
        for d in range(1, far_count)
    ]

    loads = [
        pltpu.make_async_copy(src, dst, in_sem.at[i])
        for i, (src, dst) in enumerate(
            [
                (tok_h, tok),
                (wv_h, wv),
                (wk_h, wk),
                (om_h, om),
                (wq_h, wq),
                (ck_h, ck),
                (gain_h, gain),
                (wo_h, wo),
            ]
        )
    ]
    for load in loads:
        load.start()

    barrier = pltpu.get_barrier_semaphore()
    greeted = [partner, above, below] + [base + j * CORES for _, j in near_ids] + far_ids
    for other in greeted:
        pl.semaphore_signal(barrier, inc=1, device_id={"row": other}, device_id_type=MESH)

    for s in range(2):
        for p in range(pairs):
            omp[p, s, (1 - s) * dim_head : (2 - s) * dim_head, :] = jnp.zeros((dim_head, nfeat), BF16)
            omp[p, s, lanes:, :] = jnp.ones((lanes, nfeat), BF16)
    for p in range(pairs):
        vt[p, lanes:, :] = jnp.ones((vt.shape[1] - lanes, tokens), BF16)
    for h in range(2):
        for j in range(NEAR):
            send0[h, j, KV_ROWS:, :] = jnp.zeros((CHUNK - KV_ROWS, half), BF16)

    loads[0].wait()
    loads[1].wait()
    for c in range(0, width, 256):
        vext[tokens // rows_here : tokens // rows_here + tokens, c : c + 256] = dot(
            tok[...], wv[:, c : c + 256]
        ).astype(BF16)
    loads[2].wait()
    for c in range(0, width, 256):
        proj[:, c : c + 256] = dot(tok[...], wk[:, c : c + 256]).astype(BF16)
    loads[3].wait()
    for p in range(pairs):
        for s in range(2):
            omp[p, s, s * dim_head : (s + 1) * dim_head, :] = om[2 * p + s]
        vt[p, :lanes, :] = vext[cols : cols + tokens, p * lanes : (p + 1) * lanes].T

    for p in range(pairs):
        u = proj[:, p * lanes : (p + 1) * lanes]
        feats = features(u, [omp[p, 0], omp[p, 1]], kappa, lift, dim_head)
        for s in range(2):
            head = 2 * p + s
            st = dot(vt[p], feats[s])
            for h in range(2):
                part = st[:, h * half : (h + 1) * half].astype(BF16)
                for i in range(dim_head // 16):
                    block = head * (dim_head // 16) + i
                    chunk, place = divmod(block, KV_ROWS // 16)
                    send0[h, chunk, place * 16 : (place + 1) * 16, :] = part[
                        s * dim_head + i * 16 : s * dim_head + (i + 1) * 16
                    ]
                send0[h, head + head // 3, KV_ROWS:, :] = part[lanes : lanes + 16]

    pl.semaphore_wait(barrier, len(greeted))

    swap = pltpu.make_async_remote_copy(
        src_ref=send0.at[1 - core],
        dst_ref=recv0,
        send_sem=pair_sem.at[0],
        recv_sem=pair_sem.at[1],
        device_id={"row": partner},
        device_id_type=MESH,
    )
    swap.start()
    swap.wait()
    for j in range(NEAR):
        send1[j] = (send0[core, j].astype(F32) + recv0[j].astype(F32)).astype(BF16)

    near_copies = []
    for k, (step, j) in enumerate(near_ids):
        copy = pltpu.make_async_remote_copy(
            src_ref=send1.at[j],
            dst_ref=recv1.at[k],
            send_sem=rs_sem.at[0, k],
            recv_sem=rs_sem.at[1, k],
            device_id={"row": base + j * CORES},
            device_id_type=MESH,
        )
        copy.start()
        near_copies.append(copy)

    halo_copies = []
    for k, (row, other) in enumerate([(rows_here - 1, below), (0, above)]):
        copy = pltpu.make_async_remote_copy(
            src_ref=tok.at[pl.ds(row * cols, cols)],
            dst_ref=halo.at[k],
            send_sem=halo_sem.at[0, k],
            recv_sem=halo_sem.at[1, k],
            device_id={"row": other},
            device_id_type=MESH,
        )
        copy.start()
        halo_copies.append(copy)

    loads[4].wait()
    for c in range(0, width, 256):
        proj[:, c : c + 256] = dot(tok[...], wq[:, c : c + 256]).astype(BF16)
    for p in range(pairs):
        u = proj[:, p * lanes : (p + 1) * lanes]
        feats = features(u, [omp[p, 0], omp[p, 1]], kappa, lift, dim_head)
        for s in range(2):
            fq[:, (2 * p + s) * nfeat : (2 * p + s + 1) * nfeat] = feats[s]

    for copy in near_copies:
        copy.wait()
    total = send1[near].astype(F32)
    for k in range(len(STEPS)):
        total = total + recv1[k].astype(F32)
    send2[...] = total.astype(BF16)

    far_copies = []
    for k, other in enumerate(far_ids):
        copy = pltpu.make_async_remote_copy(
            src_ref=send2,
            dst_ref=recv2.at[k],
            send_sem=far_sem.at[0, k],
            recv_sem=far_sem.at[1, k],
            device_id={"row": other},
            device_id_type=MESH,
        )
        copy.start()
        far_copies.append(copy)

    for copy in halo_copies:
        copy.wait()
    for k, (edge, place) in enumerate([(0, 0), (n - 1, rows_here + 1)]):
        rows = halo[k]
        rows = jnp.where(me == edge, jnp.zeros_like(rows), rows)
        for c in range(0, width, 256):
            vext[place * cols : (place + 1) * cols, c : c + 256] = dot(rows, wv[:, c : c + 256]).astype(
                BF16
            )
    loads[5].wait()
    column = lax.broadcasted_iota(jnp.int32, (cols, lanes), 0)
    for c in range(0, width, lanes):
        for r in range(rows_here):
            rows = [
                vext[(r + a) * cols : (r + a + 1) * cols, c : c + lanes].astype(F32) for a in range(3)
            ]
            taps = []
            for b in range(3):
                tap = rows[0] * ck[b : b + 1, c : c + lanes]
                for a in (1, 2):
                    tap = tap + rows[a] * ck[3 * a + b : 3 * a + b + 1, c : c + lanes]
                taps.append(tap)
            left = jnp.where(column == 0, 0.0, pltpu.roll(taps[0], 1, 0))
            right = jnp.where(column == cols - 1, 0.0, pltpu.roll(taps[2], cols - 1, 0))
            pos[r * cols : (r + 1) * cols, c : c + lanes] = left + taps[1] + right

    for copy in far_copies:
        copy.wait()
    total = send2[...].astype(F32)
    for k in range(len(far_ids)):
        total = total + recv2[k].astype(F32)
    state[core, near] = total.astype(BF16)

    gathers = []
    for k, (step, j) in enumerate(near_ids):
        copy = pltpu.make_async_remote_copy(
            src_ref=state.at[core, near],
            dst_ref=state.at[core, near],
            send_sem=ag_sem.at[0, k],
            recv_sem=ag_sem.at[1, k],
            device_id={"row": base + j * CORES},
            device_id_type=MESH,
        )
        copy.start()
        gathers.append(copy)

    def hand_on(j, k):
        copy = pltpu.make_async_remote_copy(
            src_ref=state.at[core, j],
            dst_ref=state.at[core, j],
            send_sem=fw_sem.at[0, k],
            recv_sem=fw_sem.at[1, k],
            device_id={"row": partner},
            device_id_type=MESH,
        )
        copy.start()
        return copy

    handed = [hand_on(near, len(STEPS))]
    for k in reversed(range(len(STEPS))):
        a, b = STEPS[k]
        gathers[k].wait()
        handed.append(hand_on(near_peer(zl, x, a, back_step(b)), k))
    for copy in handed:
        copy.wait()

    blank = jnp.zeros((dim_head, half), BF16)
    for p in range(pairs):
        for h in range(2):
            parts, sums = [], []
            for s in range(2):
                head = 2 * p + s
                blocks = []
                for i in range(dim_head // 16):
                    chunk, place = divmod(head * (dim_head // 16) + i, KV_ROWS // 16)
                    blocks.append(state[h, chunk, place * 16 : (place + 1) * 16, :])
                parts.append(jnp.concatenate(blocks, axis=0))
                key_sum = state[h, head + head // 3, KV_ROWS:, :]
                sums.append(jnp.concatenate([key_sum] * (dim_head // 16), axis=0))
            for s in range(2):
                at = (2 * h + s) * half
                for i, block in enumerate([parts, sums]):
                    for t in range(2):
                        rhs[p, (2 * i + t) * dim_head : (2 * i + t + 1) * dim_head, at : at + half] = (
                            block[s] if s == t else blank
                        )

    loads[6].wait()
    loads[7].wait()
    for r in range(rows_here):
        at = slice(r * cols, (r + 1) * cols)
        squares = jnp.zeros((cols, lanes), F32)
        for p in range(pairs):
            lhs = jnp.concatenate(
                [
                    fq[at, (2 * p + s) * nfeat + h * half : (2 * p + s) * nfeat + (h + 1) * half]
                    for h in range(2)
                    for s in range(2)
                ],
                axis=1,
            )
            both = dot_t(lhs, rhs[p])
            ratio = both[:, :lanes] / both[:, lanes:]
            attn[:, p * lanes : (p + 1) * lanes] = ratio
            squares = squares + ratio * ratio
        scale = lax.rsqrt(jnp.sum(squares, axis=1, keepdims=True) * (1.0 / width) + 1e-06)
        for c in range(0, width, lanes):
            normed = attn[:, c : c + lanes] * scale * gain[:, c : c + lanes]
            mixed[:, c : c + lanes] = (normed + pos[at, c : c + lanes]).astype(BF16)
        for c in range(0, width, 256):
            outv[at, c : c + 256] = (
                tok[at, c : c + 256].astype(F32) + dot(mixed[...], wo[:, c : c + 256])
            ).astype(BF16)
        pltpu.make_async_copy(outv.at[at], out_h.at[at], out_sem.at[r]).start()
    for r in range(rows_here):
        at = slice(r * cols, (r + 1) * cols)
        pltpu.make_async_copy(outv.at[at], out_h.at[at], out_sem.at[r]).wait()


def layer(n, tokens, w_query, w_key, w_value, w_out, omega, conv_kernel, norm_gain):
    rows_here, cols, width = tokens.shape
    heads, dim_head, nfeat = omega.shape
    count = rows_here * cols
    pairs, lanes, half = heads // 2, 2 * dim_head, nfeat // 2
    far = n // (CORES * NEAR) - 1
    steps = len(STEPS)
    vmem = pltpu.VMEM
    dma = pltpu.SemaphoreType.DMA
    out = pl.pallas_call(
        functools.partial(kernel, n, heads),
        out_shape=jax.ShapeDtypeStruct((count, width), BF16),
        in_specs=[pl.BlockSpec(memory_space=pl.ANY)] * 8,
        out_specs=pl.BlockSpec(memory_space=pl.ANY),
        scratch_shapes=[
            vmem((count, width), BF16),
            vmem((width, width), BF16),
            vmem((width, width), BF16),
            vmem((width, width), BF16),
            vmem((width, width), BF16),
            vmem((heads, dim_head, nfeat), BF16),
            vmem((9, width), F32),
            vmem((1, width), F32),
            vmem((pairs, 2, 2 * lanes, nfeat), BF16),
            vmem((count, width), BF16),
            vmem((count + 2 * cols, width), BF16),
            vmem((2, cols, width), BF16),
            vmem((pairs, lanes + 16, count), BF16),
            vmem((count, heads * nfeat), BF16),
            vmem((count, width), F32),
            vmem((cols, width), F32),
            vmem((cols, width), BF16),
            vmem((count, width), BF16),
            vmem((2, NEAR, CHUNK, half), BF16),
            vmem((NEAR, CHUNK, half), BF16),
            vmem((NEAR, CHUNK, half), BF16),
            vmem((steps, CHUNK, half), BF16),
            vmem((CHUNK, half), BF16),
            vmem((far, CHUNK, half), BF16),
            vmem((2, NEAR, CHUNK, half), BF16),
            vmem((pairs, 2 * lanes, 2 * nfeat), BF16),
            dma((8,)),
            dma((rows_here,)),
            dma((2,)),
            dma((2, 2)),
            dma((2, steps)),
            dma((2, far)),
            dma((2, steps)),
            dma((2, steps + 1)),
        ],
        compiler_params=pltpu.CompilerParams(
            collective_id=0, has_side_effects=True, vmem_limit_bytes=56 * 1024 * 1024
        ),
        name="favor_layer",
    )(
        tokens.reshape(count, width),
        w_query,
        w_key,
        w_value,
        w_out,
        omega,
        conv_kernel.reshape(9, width),
        norm_gain.reshape(1, width),
    )
    return out.reshape(rows_here, cols, width)


def solution(mesh):
    return jax.shard_map(
        functools.partial(layer, mesh.shape["row"]),
        mesh=mesh,
        in_specs=(P(("parts", "row"), None, None), P(), P(), P(), P(), P(), P(), P()),
        out_specs=P(("parts", "row"), None, None),
        check_vma=False,
    )
```

```python
import functools
import math

import jax
import jax.numpy as jnp
from jax import lax
from jax.experimental import pallas as pl
from jax.experimental.pallas import tpu as pltpu
from jax.sharding import PartitionSpec as P

MESH = pl.DeviceIdType.MESH
F32 = jnp.float32
BF16 = jnp.bfloat16

XS = 4
ZN = 4
CORES = 2
NEAR = XS * ZN
KV_ROWS = 48
CHUNK = 56


def near_peer(zl, x, a, b):
    if a == 0:
        zp = zl
    elif a == 1:
        zp = zl + 1 - 2 * (zl % 2)
    elif a == 2:
        zp = (zl + 2) % 4
    else:
        zp = 3 - zl
    return zp * XS + (x + b) % XS


STEPS = [(a, b) for a in (3, 2, 1) for b in (2, 1, 3, 0)] + [(0, b) for b in (2, 1, 3)]


def back_step(b):
    return (XS - b) % XS


def dot(a, b):
    return jnp.dot(a, b, preferred_element_type=F32)


def dot_t(a, b):
    return lax.dot_general(a, b, (((1,), (1,)), ((), ())), preferred_element_type=F32)


def features(u, omega_pad, kappa, lift, dim_head):
    nfeat = omega_pad[0].shape[-1]
    u32 = u.astype(F32)
    square = u32 * u32 * (-lift) - (0.5 * math.log2(nfeat) / kappa / dim_head)
    high = square.astype(BF16).astype(F32)
    low = pltpu.roll(square - high, dim_head, 1)
    first = lax.broadcasted_iota(jnp.int32, square.shape, 1) < dim_head
    out = []
    for s in range(2):
        parts = jnp.where(first, high, low) if s == 0 else jnp.where(first, low, high)
        lhs = jnp.concatenate([u, parts.astype(BF16)], axis=1)
        arg = dot(lhs, omega_pad[s])
        out.append(jnp.exp2(arg * kappa).astype(BF16))
    return out


def kernel(
    n,
    heads,
    tok_h,
    wq_h,
    wk_h,
    wv_h,
    wo_h,
    om_h,
    ck_h,
    gain_h,
    out,
    tok,
    wq,
    wk,
    wv,
    wo,
    om,
    ck,
    gain,
    omp,
    proj,
    vext,
    halo,
    vt,
    fq,
    pos,
    attn,
    mixed,
    send0,
    recv0,
    send1,
    recv1,
    send2,
    recv2,
    state,
    rhs,
    in_sem,
    pair_sem,
    halo_sem,
    rs_sem,
    far_sem,
    ag_sem,
    fw_sem,
    relay_sem,
):
    tokens, width = tok.shape
    cols = halo.shape[1]
    rows_here = tokens // cols
    dim_head = width // heads
    nfeat = om.shape[-1]
    pairs = heads // 2
    lanes = 2 * dim_head
    half = nfeat // 2
    kappa = dim_head ** (-0.25) * math.log2(math.e)
    lift = 0.5 * dim_head ** (-0.5) / dim_head ** (-0.25)

    me = lax.axis_index("row")
    core = me % CORES
    near = (me // CORES) % NEAR
    zl, x = near // XS, near % XS
    far_count = n // (CORES * NEAR)
    far = me // (CORES * NEAR)
    base = far * (CORES * NEAR) + core

    partner = me + 1 - 2 * core
    above, below = (me + n - 1) % n, (me + 1) % n
    near_ids = [(s, near_peer(zl, x, *s)) for s in STEPS]
    far_ids = [
        ((far + d) % far_count) * (CORES * NEAR) + near * CORES + core
        for d in range(1, far_count)
    ]
    next_ids = [far_ids[0], far_ids[-1]]

    barrier = pltpu.get_barrier_semaphore()
    greeted = next_ids + [base + j * CORES for _, j in near_ids] + [above, below, partner]
    for other in greeted:
        pl.semaphore_signal(barrier, inc=1, device_id={"row": other}, device_id_type=MESH)

    blocks = [slice(c, c + 256) for c in range(0, width, 256)]

    def load(src, dst, i):
        copy = pltpu.make_async_copy(src, dst, in_sem.at[i])
        copy.start()
        return copy

    parts = [slice(i * width // 2, (i + 1) * width // 2) for i in range(2)]
    tok_loads = [
        load(tok_h.at[pl.ds(i * cols, cols)], tok.at[pl.ds(i * cols, cols)], i) for i in range(rows_here)
    ]
    v_loads = [load(wv_h.at[part], wv.at[part], rows_here + i) for i, part in enumerate(parts)]
    k_loads = [load(wk_h.at[part], wk.at[part], rows_here + 2 + i) for i, part in enumerate(parts)]
    om_load = load(om_h, om, rows_here + 4)

    for s in range(2):
        for p in range(pairs):
            omp[p, s, (1 - s) * dim_head : (2 - s) * dim_head, :] = jnp.zeros((dim_head, nfeat), BF16)
            omp[p, s, lanes:, :] = jnp.ones((lanes, nfeat), BF16)
    for p in range(pairs):
        vt[p, lanes:, :] = jnp.ones((vt.shape[1] - lanes, tokens), BF16)
    for h in range(2):
        for j in range(NEAR):
            send0[h, j, KV_ROWS:, :] = jnp.zeros((CHUNK - KV_ROWS, half), BF16)

    for copy in tok_loads + v_loads:
        copy.wait()
    for block in blocks:
        vext[cols : cols + tokens, block] = dot(tok[...], wv[:, block]).astype(BF16)
    for copy in k_loads:
        copy.wait()
    for block in blocks:
        proj[:, block] = dot(tok[...], wk[:, block]).astype(BF16)
    om_load.wait()
    late = rows_here + 5
    q_load = load(wq_h, wq, late)
    ck_load = load(ck_h, ck, late + 1)
    gain_load = load(gain_h, gain, late + 2)
    o_load = load(wo_h, wo, late + 3)
    for p in range(pairs):
        for s in range(2):
            omp[p, s, s * dim_head : (s + 1) * dim_head, :] = om[2 * p + s]
        vt[p, :lanes, :] = vext[cols : cols + tokens, p * lanes : (p + 1) * lanes].T

    for p in range(pairs):
        u = proj[:, p * lanes : (p + 1) * lanes]
        feats = features(u, [omp[p, 0], omp[p, 1]], kappa, lift, dim_head)
        for s in range(2):
            head = 2 * p + s
            st = dot(vt[p], feats[s])
            for h in range(2):
                part = st[:, h * half : (h + 1) * half].astype(BF16)
                for i in range(dim_head // 16):
                    block = head * (dim_head // 16) + i
                    chunk, place = divmod(block, KV_ROWS // 16)
                    send0[h, chunk, place * 16 : (place + 1) * 16, :] = part[
                        s * dim_head + i * 16 : s * dim_head + (i + 1) * 16
                    ]
                send0[h, head + head // 3, KV_ROWS:, :] = part[lanes : lanes + CHUNK - KV_ROWS]

    pl.semaphore_wait(barrier, len(greeted))
    for other in next_ids:
        pl.semaphore_signal(relay_sem, inc=1, device_id={"row": other}, device_id_type=MESH)

    swap = pltpu.make_async_remote_copy(
        src_ref=send0.at[1 - core],
        dst_ref=recv0,
        send_sem=pair_sem.at[0],
        recv_sem=pair_sem.at[1],
        device_id={"row": partner},
        device_id_type=MESH,
    )
    swap.start()
    swap.wait()
    for j in range(NEAR):
        send1[j] = (send0[core, j].astype(F32) + recv0[j].astype(F32)).astype(BF16)

    near_copies = []
    for k, (step, j) in enumerate(near_ids):
        copy = pltpu.make_async_remote_copy(
            src_ref=send1.at[j],
            dst_ref=recv1.at[k],
            send_sem=rs_sem.at[0, k],
            recv_sem=rs_sem.at[1, k],
            device_id={"row": base + j * CORES},
            device_id_type=MESH,
        )
        copy.start()
        near_copies.append(copy)

    halo_copies = []
    for k, (row, other) in enumerate([(rows_here - 1, below), (0, above)]):
        copy = pltpu.make_async_remote_copy(
            src_ref=tok.at[pl.ds(row * cols, cols)],
            dst_ref=halo.at[k],
            send_sem=halo_sem.at[0, k],
            recv_sem=halo_sem.at[1, k],
            device_id={"row": other},
            device_id_type=MESH,
        )
        copy.start()
        halo_copies.append(copy)

    q_load.wait()
    for c in range(0, width, 256):
        proj[:, c : c + 256] = dot(tok[...], wq[:, c : c + 256]).astype(BF16)
    for p in range(pairs):
        u = proj[:, p * lanes : (p + 1) * lanes]
        feats = features(u, [omp[p, 0], omp[p, 1]], kappa, lift, dim_head)
        for s in range(2):
            fq[:, (2 * p + s) * nfeat : (2 * p + s + 1) * nfeat] = feats[s]

    for copy in near_copies:
        copy.wait()
    total = send1[near].astype(F32)
    for k in range(len(STEPS)):
        total = total + recv1[k].astype(F32)
    send2[...] = total.astype(BF16)

    pl.semaphore_wait(relay_sem, len(next_ids))
    far_copies = []
    for k, other in sorted(enumerate(far_ids), key=lambda item: abs(2 * item[0] + 2 - far_count)):
        copy = pltpu.make_async_remote_copy(
            src_ref=send2,
            dst_ref=recv2.at[k],
            send_sem=far_sem.at[0, k],
            recv_sem=far_sem.at[1, k],
            device_id={"row": other},
            device_id_type=MESH,
        )
        copy.start()
        far_copies.append(copy)

    for copy in halo_copies:
        copy.wait()
    for k, (edge, place) in enumerate([(0, 0), (n - 1, rows_here + 1)]):
        rows = halo[k]
        rows = jnp.where(me == edge, jnp.zeros_like(rows), rows)
        for c in range(0, width, 256):
            vext[place * cols : (place + 1) * cols, c : c + 256] = dot(rows, wv[:, c : c + 256]).astype(
                BF16
            )
    ck_load.wait()
    column = lax.broadcasted_iota(jnp.int32, (cols, lanes), 0)
    for c in range(0, width, lanes):
        for r in range(rows_here):
            rows = [
                vext[(r + a) * cols : (r + a + 1) * cols, c : c + lanes].astype(F32) for a in range(3)
            ]
            taps = []
            for b in range(3):
                tap = rows[0] * ck[0, b : b + 1, c : c + lanes]
                for a in (1, 2):
                    tap = tap + rows[a] * ck[a, b : b + 1, c : c + lanes]
                taps.append(tap)
            left = jnp.where(column == 0, 0.0, pltpu.roll(taps[0], 1, 0))
            right = jnp.where(column == cols - 1, 0.0, pltpu.roll(taps[2], cols - 1, 0))
            pos[r * cols : (r + 1) * cols, c : c + lanes] = left + taps[1] + right

    for copy in far_copies:
        copy.wait()
    total = send2[...].astype(F32)
    for k in range(len(far_ids)):
        total = total + recv2[k].astype(F32)
    state[core, near] = total.astype(BF16)

    gathers = []
    for k, (step, j) in enumerate(near_ids):
        copy = pltpu.make_async_remote_copy(
            src_ref=state.at[core, near],
            dst_ref=state.at[core, near],
            send_sem=ag_sem.at[0, k],
            recv_sem=ag_sem.at[1, k],
            device_id={"row": base + j * CORES},
            device_id_type=MESH,
        )
        copy.start()
        gathers.append(copy)

    def hand_on(j, k):
        copy = pltpu.make_async_remote_copy(
            src_ref=state.at[core, j],
            dst_ref=state.at[core, j],
            send_sem=fw_sem.at[0, k],
            recv_sem=fw_sem.at[1, k],
            device_id={"row": partner},
            device_id_type=MESH,
        )
        copy.start()
        return copy

    handed = [hand_on(near, len(STEPS))]
    for k in reversed(range(len(STEPS))):
        a, b = STEPS[k]
        gathers[k].wait()
        handed.append(hand_on(near_peer(zl, x, a, back_step(b)), k))
    for copy in handed:
        copy.wait()

    blank = jnp.zeros((dim_head, half), BF16)
    for p in range(pairs):
        for h in range(2):
            parts, sums = [], []
            for s in range(2):
                head = 2 * p + s
                blocks = []
                for i in range(dim_head // 16):
                    chunk, place = divmod(head * (dim_head // 16) + i, KV_ROWS // 16)
                    blocks.append(state[h, chunk, place * 16 : (place + 1) * 16, :])
                parts.append(jnp.concatenate(blocks, axis=0))
                key_sum = state[h, head + head // 3, KV_ROWS:, :]
                sums.append(jnp.concatenate([key_sum] * (dim_head // (CHUNK - KV_ROWS)), axis=0))
            for s in range(2):
                at = (2 * h + s) * half
                for i, block in enumerate([parts, sums]):
                    for t in range(2):
                        rhs[p, (2 * i + t) * dim_head : (2 * i + t + 1) * dim_head, at : at + half] = (
                            block[s] if s == t else blank
                        )

    gain_load.wait()
    o_load.wait()
    for r in range(rows_here):
        at = slice(r * cols, (r + 1) * cols)
        squares = jnp.zeros((cols, lanes), F32)
        for p in range(pairs):
            lhs = jnp.concatenate(
                [
                    fq[at, (2 * p + s) * nfeat + h * half : (2 * p + s) * nfeat + (h + 1) * half]
                    for h in range(2)
                    for s in range(2)
                ],
                axis=1,
            )
            both = dot_t(lhs, rhs[p])
            ratio = both[:, :lanes] / both[:, lanes:]
            attn[at, p * lanes : (p + 1) * lanes] = ratio
            squares = squares + ratio * ratio
        scale = lax.rsqrt(jnp.sum(squares, axis=1, keepdims=True) * (1.0 / width) + 1e-06)
        for c in range(0, width, lanes):
            normed = attn[at, c : c + lanes] * scale * gain[c : c + lanes].reshape(1, lanes)
            mixed[at, c : c + lanes] = (normed + pos[at, c : c + lanes]).astype(BF16)
        for c in range(0, width, 256):
            out[at, c : c + 256] = (
                tok[at, c : c + 256].astype(F32) + dot(mixed[at], wo[:, c : c + 256])
            ).astype(BF16)


def layer(n, tokens, w_query, w_key, w_value, w_out, omega, conv_kernel, norm_gain):
    rows_here, cols, width = tokens.shape
    heads, dim_head, nfeat = omega.shape
    count = rows_here * cols
    pairs, lanes, half = heads // 2, 2 * dim_head, nfeat // 2
    far = n // (CORES * NEAR) - 1
    steps = len(STEPS)
    vmem = pltpu.VMEM
    dma = pltpu.SemaphoreType.DMA
    out = pl.pallas_call(
        functools.partial(kernel, n, heads),
        out_shape=jax.ShapeDtypeStruct((count, width), BF16),
        in_specs=[pl.BlockSpec(memory_space=pl.ANY)] * 8,
        out_specs=pl.BlockSpec(memory_space=pltpu.VMEM),
        scratch_shapes=[
            vmem((count, width), BF16),
            vmem((width, width), BF16),
            vmem((width, width), BF16),
            vmem((width, width), BF16),
            vmem((width, width), BF16),
            vmem((heads, dim_head, nfeat), BF16),
            vmem((3, 3, width), F32),
            vmem((width,), F32),
            vmem((pairs, 2, 2 * lanes, nfeat), BF16),
            vmem((count, width), BF16),
            vmem((count + 2 * cols, width), BF16),
            vmem((2, cols, width), BF16),
            vmem((pairs, lanes + 16, count), BF16),
            vmem((count, heads * nfeat), BF16),
            vmem((count, width), F32),
            vmem((count, width), F32),
            vmem((count, width), BF16),
            vmem((2, NEAR, CHUNK, half), BF16),
            vmem((NEAR, CHUNK, half), BF16),
            vmem((NEAR, CHUNK, half), BF16),
            vmem((steps, CHUNK, half), BF16),
            vmem((CHUNK, half), BF16),
            vmem((far, CHUNK, half), BF16),
            vmem((2, NEAR, CHUNK, half), BF16),
            vmem((pairs, 2 * lanes, 2 * nfeat), BF16),
            dma((rows_here + 9,)),
            dma((2,)),
            dma((2, 2)),
            dma((2, steps)),
            dma((2, far)),
            dma((2, steps)),
            dma((2, steps + 1)),
            pltpu.SemaphoreType.REGULAR,
        ],
        compiler_params=pltpu.CompilerParams(
            collective_id=0, has_side_effects=True, vmem_limit_bytes=48 * 1024 * 1024
        ),
        name="favor_layer",
    )(
        *[
            pltpu.with_memory_space_constraint(operand, pltpu.HBM)
            for operand in (
                tokens.reshape(count, width),
                w_query,
                w_key,
                w_value,
                w_out,
                omega,
                conv_kernel,
                norm_gain,
            )
        ]
    )
    return out.reshape(rows_here, cols, width)


def solution(mesh):
    return jax.shard_map(
        functools.partial(layer, mesh.shape["row"]),
        mesh=mesh,
        in_specs=(P(("parts", "row"), None, None), P(), P(), P(), P(), P(), P(), P()),
        out_specs=P(("parts", "row"), None, None),
        check_vma=False,
    )
```

```python
import functools
import math

import jax
import jax.numpy as jnp
from jax import lax
from jax.experimental import pallas as pl
from jax.experimental.pallas import tpu as pltpu
from jax.sharding import PartitionSpec as P

MESH = pl.DeviceIdType.MESH
F32 = jnp.float32
BF16 = jnp.bfloat16

XS = 4
ZN = 4
CORES = 2
NEAR = XS * ZN
KV_ROWS = 48
CHUNK = 56


def slot(zl, x):
    return (zl + x) % 2 * (NEAR // 2) + zl * (XS // 2) + x // 2


def run_step(zl, a):
    return [zl, zl + 1 - 2 * (zl % 2), (zl + 2) % ZN, ZN - 1 - zl][a]


STEPS = [(a, b) for a in (3, 2, 1) for b in (2, 1, 3, 0)] + [(0, b) for b in (2, 1, 3)]


def dot(a, b):
    return jnp.dot(a, b, preferred_element_type=F32)


def dot_t(a, b):
    return lax.dot_general(a, b, (((1,), (1,)), ((), ())), preferred_element_type=F32)


def features(u, omega_pad, kappa, lift, dim_head):
    nfeat = omega_pad[0].shape[-1]
    u32 = u.astype(F32)
    square = u32 * u32 * (-lift) - (0.5 * math.log2(nfeat) / kappa / dim_head)
    high = square.astype(BF16).astype(F32)
    low = pltpu.roll(square - high, dim_head, 1)
    first = lax.broadcasted_iota(jnp.int32, square.shape, 1) < dim_head
    out = []
    for s in range(2):
        parts = jnp.where(first, high, low) if s == 0 else jnp.where(first, low, high)
        lhs = jnp.concatenate([u, parts.astype(BF16)], axis=1)
        arg = dot(lhs, omega_pad[s])
        out.append(jnp.exp2(arg * kappa).astype(BF16))
    return out


def kernel(
    n,
    heads,
    tok_h,
    wq_h,
    wk_h,
    wv_h,
    wo_h,
    om_h,
    ck_h,
    gain_h,
    out,
    tok,
    wq,
    wk,
    wv,
    wo,
    om,
    ck,
    gain,
    omp,
    proj,
    vext,
    halo,
    vt,
    fq,
    pos,
    attn,
    mixed,
    send0,
    recv0,
    send1,
    recv1,
    send2,
    recv2,
    state,
    rhs,
    partial,
    in_sem,
    pair_sem,
    halo_sem,
    rs_sem,
    far_sem,
    ag_sem,
    fw_sem,
    relay_sem,
):
    tokens, width = tok.shape
    cols = halo.shape[1]
    rows_here = tokens // cols
    dim_head = width // heads
    nfeat = om.shape[-1]
    pairs = heads // 2
    lanes = 2 * dim_head
    half = nfeat // 2
    kappa = dim_head ** (-0.25) * math.log2(math.e)
    lift = 0.5 * dim_head ** (-0.5) / dim_head ** (-0.25)

    me = lax.axis_index("row")
    core = me % CORES
    x = (me // CORES) % XS
    z_count = n // (CORES * XS)
    far_count = z_count // ZN
    shift = core * (ZN // 2)
    z = (me // (CORES * XS) + shift) % z_count
    zl, far = z % ZN, z // ZN
    near = slot(zl, x)

    def device(run, zl, x):
        return (((run * ZN + zl + z_count - shift) % z_count) * XS + x) * CORES + core

    partner = me + 1 - 2 * core
    above, below = (me + n - 1) % n, (me + 1) % n
    near_to = [(run_step(zl, a), (x + b) % XS) for a, b in STEPS]
    near_from = [(run_step(zl, a), (x + XS - b) % XS) for a, b in STEPS]
    far_ids = [device((far + d) % far_count, zl, x) for d in range(1, far_count)]
    next_ids = [far_ids[0], far_ids[-1]]

    blocks = [slice(c, c + 256) for c in range(0, width, 256)]

    def load(src, dst, i):
        copy = pltpu.make_async_copy(src, dst, in_sem.at[i])
        copy.start()
        return copy

    parts = [slice(i * width // 2, (i + 1) * width // 2) for i in range(2)]
    tok_loads = [
        load(tok_h.at[pl.ds(i * cols, cols)], tok.at[pl.ds(i * cols, cols)], i) for i in range(rows_here)
    ]
    v_loads = [load(wv_h.at[part], wv.at[part], rows_here + i) for i, part in enumerate(parts)]
    k_loads = [load(wk_h.at[part], wk.at[part], rows_here + 2 + i) for i, part in enumerate(parts)]
    om_load = load(om_h, om, rows_here + 4)

    barrier = pltpu.get_barrier_semaphore()
    greeted = next_ids + [device(far, *to) for to in near_to] + [above, below, partner]
    for other in greeted:
        pl.semaphore_signal(barrier, inc=1, device_id={"row": other}, device_id_type=MESH)

    for s in range(2):
        for p in range(pairs):
            omp[p, s, (1 - s) * dim_head : (2 - s) * dim_head, :] = jnp.zeros((dim_head, nfeat), BF16)
            omp[p, s, lanes:, :] = jnp.ones((lanes, nfeat), BF16)
    for p in range(pairs):
        vt[p, lanes:, :] = jnp.ones((vt.shape[1] - lanes, tokens), BF16)
    for h in range(2):
        for j in range(NEAR):
            send0[h, j, KV_ROWS:, :] = jnp.zeros((CHUNK - KV_ROWS, half), BF16)

    for copy in tok_loads + v_loads:
        copy.wait()
    for block in blocks:
        vext[cols : cols + tokens, block] = dot(tok[...], wv[:, block]).astype(BF16)
    for copy in k_loads:
        copy.wait()
    for block in blocks:
        proj[:, block] = dot(tok[...], wk[:, block]).astype(BF16)
    om_load.wait()
    late = rows_here + 5
    q_load = load(wq_h, wq, late)
    ck_load = load(ck_h, ck, late + 1)
    gain_load = load(gain_h, gain, late + 2)
    o_load = load(wo_h, wo, late + 3)
    for p in range(pairs):
        for s in range(2):
            omp[p, s, s * dim_head : (s + 1) * dim_head, :] = om[2 * p + s]
        vt[p, :lanes, :] = vext[cols : cols + tokens, p * lanes : (p + 1) * lanes].T

    def local(own_pairs):
        for p in own_pairs:
            u = proj[:, p * lanes : (p + 1) * lanes]
            feats = features(u, [omp[p, 0], omp[p, 1]], kappa, lift, dim_head)
            for s in range(2):
                head = 2 * p + s
                st = dot(vt[p], feats[s])
                for h in range(2):
                    part = st[:, h * half : (h + 1) * half].astype(BF16)
                    for i in range(dim_head // 16):
                        block = head * (dim_head // 16) + i
                        chunk, place = divmod(block, KV_ROWS // 16)
                        send0[h, chunk, place * 16 : (place + 1) * 16, :] = part[
                            s * dim_head + i * 16 : s * dim_head + (i + 1) * 16
                        ]
                    send0[h, head + head // 3, KV_ROWS:, :] = part[lanes : lanes + CHUNK - KV_ROWS]

    def swap(wave):
        own = pl.ds(wave * NEAR // 2, NEAR // 2)
        copy = pltpu.make_async_remote_copy(
            src_ref=send0.at[1 - core, own],
            dst_ref=recv0.at[own],
            send_sem=pair_sem.at[0, wave],
            recv_sem=pair_sem.at[1, wave],
            device_id={"row": partner},
            device_id_type=MESH,
        )
        copy.start()
        return copy

    def scatter_copy(to, source, place):
        return pltpu.make_async_remote_copy(
            src_ref=send1.at[slot(*to)],
            dst_ref=recv1.at[place],
            send_sem=rs_sem.at[0, slot(*to)],
            recv_sem=rs_sem.at[1, source],
            device_id={"row": device(far, *to)},
            device_id_type=MESH,
        )

    def scatter(wave):
        for a in (3, 2, 1, 0):
            zp = run_step(zl, a)
            odd = (wave + zp + x) % 2
            for b in (2, 0):
                to = (zp, (x + odd + b) % XS)
                j = slot(*to)
                send1[j] = (send0[core, j].astype(F32) + recv0[j].astype(F32)).astype(BF16)
                copy = scatter_copy(to, near, near)
                if a == 0 and b == 0:
                    pl.when(odd == 1)(copy.start)
                else:
                    copy.start()

    local(range(pairs // 2))
    pl.semaphore_wait(barrier, len(greeted))
    for other in next_ids:
        pl.semaphore_signal(relay_sem, inc=1, device_id={"row": other}, device_id_type=MESH)
    first = swap(0)
    local(range(pairs // 2, pairs))
    second = swap(1)
    first.wait()
    scatter(0)
    second.wait()
    scatter(1)

    q_load.wait()
    for c in range(0, width, 256):
        proj[:, c : c + 256] = dot(tok[...], wq[:, c : c + 256]).astype(BF16)
    for p in range(pairs):
        u = proj[:, p * lanes : (p + 1) * lanes]
        feats = features(u, [omp[p, 0], omp[p, 1]], kappa, lift, dim_head)
        for s in range(2):
            for h in range(2):
                fq[h, :, (2 * p + s) * half : (2 * p + s + 1) * half] = feats[s][:, h * half : (h + 1) * half]

    for to, source in zip(near_to, near_from):
        scatter_copy(to, slot(*source), slot(*source)).wait()
    recv1[near] = send1[near]
    total = recv1[0].astype(F32)
    for k in range(1, NEAR):
        total = total + recv1[k].astype(F32)
    send2[...] = total.astype(BF16)

    pl.semaphore_wait(relay_sem, len(next_ids))
    far_copies = []
    for k, other in sorted(enumerate(far_ids), key=lambda item: abs(2 * item[0] + 2 - far_count)):
        copy = pltpu.make_async_remote_copy(
            src_ref=send2,
            dst_ref=recv2.at[k],
            send_sem=far_sem.at[0, k],
            recv_sem=far_sem.at[1, k],
            device_id={"row": other},
            device_id_type=MESH,
        )
        copy.start()
        far_copies.append(copy)

    halo_copies = []
    for k, (row, other) in enumerate([(rows_here - 1, below), (0, above)]):
        copy = pltpu.make_async_remote_copy(
            src_ref=tok.at[pl.ds(row * cols, cols)],
            dst_ref=halo.at[k],
            send_sem=halo_sem.at[0, k],
            recv_sem=halo_sem.at[1, k],
            device_id={"row": other},
            device_id_type=MESH,
        )
        copy.start()
        halo_copies.append(copy)

    for copy in far_copies:
        copy.wait()
    total = send2[...].astype(F32)
    for k in range(len(far_ids)):
        total = total + recv2[k].astype(F32)
    state[core, near] = total.astype(BF16)

    gathers = []
    for k, to in enumerate(near_to):
        copy = pltpu.make_async_remote_copy(
            src_ref=state.at[core, near],
            dst_ref=state.at[core, near],
            send_sem=ag_sem.at[0, k],
            recv_sem=ag_sem.at[1, k],
            device_id={"row": device(far, *to)},
            device_id_type=MESH,
        )
        copy.start()
        gathers.append(copy)

    for copy in halo_copies:
        copy.wait()
    for k, (edge, place) in enumerate([(0, 0), (n - 1, rows_here + 1)]):
        rows = halo[k]
        rows = jnp.where(me == edge, jnp.zeros_like(rows), rows)
        for c in range(0, width, 256):
            vext[place * cols : (place + 1) * cols, c : c + 256] = dot(rows, wv[:, c : c + 256]).astype(
                BF16
            )
    ck_load.wait()
    column = lax.broadcasted_iota(jnp.int32, (cols, lanes), 0)
    for c in range(0, width, lanes):
        for r in range(rows_here):
            rows = [
                vext[(r + a) * cols : (r + a + 1) * cols, c : c + lanes].astype(F32) for a in range(3)
            ]
            taps = []
            for b in range(3):
                tap = rows[0] * ck[0, b : b + 1, c : c + lanes]
                for a in (1, 2):
                    tap = tap + rows[a] * ck[a, b : b + 1, c : c + lanes]
                taps.append(tap)
            left = jnp.where(column == 0, 0.0, pltpu.roll(taps[0], 1, 0))
            right = jnp.where(column == cols - 1, 0.0, pltpu.roll(taps[2], cols - 1, 0))
            pos[r * cols : (r + 1) * cols, c : c + lanes] = left + taps[1] + right

    def hand_on(j, k):
        copy = pltpu.make_async_remote_copy(
            src_ref=state.at[core, j],
            dst_ref=state.at[core, j],
            send_sem=fw_sem.at[0, k],
            recv_sem=fw_sem.at[1, k],
            device_id={"row": partner},
            device_id_type=MESH,
        )
        copy.start()
        return copy

    handed = [hand_on(near, len(STEPS))]
    for k in reversed(range(len(STEPS))):
        gathers[k].wait()
        handed.append(hand_on(slot(*near_from[k]), k))
    blank = jnp.zeros((dim_head, half), BF16)

    def operand(slot, h):
        for p in range(pairs):
            parts, sums = [], []
            for s in range(2):
                head = 2 * p + s
                tiles = []
                for i in range(dim_head // 16):
                    chunk, place = divmod(head * (dim_head // 16) + i, KV_ROWS // 16)
                    tiles.append(state[h, chunk, place * 16 : (place + 1) * 16, :])
                parts.append(jnp.concatenate(tiles, axis=0))
                key_sum = state[h, head + head // 3, KV_ROWS:, :]
                sums.append(jnp.concatenate([key_sum] * (dim_head // (CHUNK - KV_ROWS)), axis=0))
            for s in range(2):
                for i, block in enumerate([parts, sums]):
                    for t in range(2):
                        rhs[slot, p, (2 * i + t) * dim_head : (2 * i + t + 1) * dim_head, s * half : (s + 1) * half] = (
                            block[s] if s == t else blank
                        )

    operand(0, core)
    for p in range(pairs):
        at = slice(p * 2 * lanes, (p + 1) * 2 * lanes)
        partial[:, at] = dot_t(fq[core, :, at], rhs[0, p])
    for copy in handed:
        copy.wait()
    operand(1, 1 - core)
    gain_load.wait()
    o_load.wait()
    for r in range(rows_here):
        at = slice(r * cols, (r + 1) * cols)
        squares = jnp.zeros((cols, lanes), F32)
        for p in range(pairs):
            on = slice(p * 2 * lanes, (p + 1) * 2 * lanes)
            both = partial[at, on] + dot_t(fq[1 - core, at, on], rhs[1, p])
            ratio = both[:, :lanes] / both[:, lanes:]
            attn[at, p * lanes : (p + 1) * lanes] = ratio
            squares = squares + ratio * ratio
        scale = lax.rsqrt(jnp.sum(squares, axis=1, keepdims=True) * (1.0 / width) + 1e-06)
        for c in range(0, width, lanes):
            normed = attn[at, c : c + lanes] * scale * gain[c : c + lanes].reshape(1, lanes)
            mixed[at, c : c + lanes] = (normed + pos[at, c : c + lanes]).astype(BF16)
        for c in range(0, width, 256):
            out[at, c : c + 256] = (
                tok[at, c : c + 256].astype(F32) + dot(mixed[at], wo[:, c : c + 256])
            ).astype(BF16)


def layer(n, tokens, w_query, w_key, w_value, w_out, omega, conv_kernel, norm_gain):
    rows_here, cols, width = tokens.shape
    heads, dim_head, nfeat = omega.shape
    count = rows_here * cols
    pairs, lanes, half = heads // 2, 2 * dim_head, nfeat // 2
    far = n // (CORES * NEAR) - 1
    steps = len(STEPS)
    vmem = pltpu.VMEM
    dma = pltpu.SemaphoreType.DMA
    out = pl.pallas_call(
        functools.partial(kernel, n, heads),
        out_shape=jax.ShapeDtypeStruct((count, width), BF16),
        in_specs=[pl.BlockSpec(memory_space=pl.ANY)] * 8,
        out_specs=pl.BlockSpec(memory_space=pltpu.VMEM),
        scratch_shapes=[
            vmem((count, width), BF16),
            vmem((width, width), BF16),
            vmem((width, width), BF16),
            vmem((width, width), BF16),
            vmem((width, width), BF16),
            vmem((heads, dim_head, nfeat), BF16),
            vmem((3, 3, width), F32),
            vmem((width,), F32),
            vmem((pairs, 2, 2 * lanes, nfeat), BF16),
            vmem((count, width), BF16),
            vmem((count + 2 * cols, width), BF16),
            vmem((2, cols, width), BF16),
            vmem((pairs, lanes + 16, count), BF16),
            vmem((2, count, heads * half), BF16),
            vmem((count, width), F32),
            vmem((count, width), F32),
            vmem((count, width), BF16),
            vmem((2, NEAR, CHUNK, half), BF16),
            vmem((NEAR, CHUNK, half), BF16),
            vmem((NEAR, CHUNK, half), BF16),
            vmem((NEAR, CHUNK, half), BF16),
            vmem((CHUNK, half), BF16),
            vmem((far, CHUNK, half), BF16),
            vmem((2, NEAR, CHUNK, half), BF16),
            vmem((2, pairs, 2 * lanes, nfeat), BF16),
            vmem((count, pairs * 2 * lanes), F32),
            dma((rows_here + 9,)),
            dma((2, 2)),
            dma((2, 2)),
            dma((2, NEAR)),
            dma((2, far)),
            dma((2, steps)),
            dma((2, steps + 1)),
            pltpu.SemaphoreType.REGULAR,
        ],
        compiler_params=pltpu.CompilerParams(
            collective_id=0, has_side_effects=True, vmem_limit_bytes=48 * 1024 * 1024
        ),
        name="favor_layer",
    )(
        *[
            pltpu.with_memory_space_constraint(operand, pltpu.HBM)
            for operand in (
                tokens.reshape(count, width),
                w_query,
                w_key,
                w_value,
                w_out,
                omega,
                conv_kernel,
                norm_gain,
            )
        ]
    )
    return out.reshape(rows_here, cols, width)


def solution(mesh):
    return jax.shard_map(
        functools.partial(layer, mesh.shape["row"]),
        mesh=mesh,
        in_specs=(P(("parts", "row"), None, None), P(), P(), P(), P(), P(), P(), P()),
        out_specs=P(("parts", "row"), None, None),
        check_vma=False,
    )
```

```python
import functools
import math

import jax
import jax.numpy as jnp
from jax import lax
from jax.experimental import pallas as pl
from jax.experimental.pallas import tpu as pltpu
from jax.sharding import PartitionSpec as P

MESH = pl.DeviceIdType.MESH
F32 = jnp.float32
BF16 = jnp.bfloat16

XS = 4
ZN = 4
CORES = 2
NEAR = XS * ZN
WAVES = XS
KV_ROWS = 48
CHUNK = 56


def slot(zl, x):
    return (zl + x) % WAVES * ZN + zl


def run_step(zl, a):
    return [zl, zl + 1 - 2 * (zl % 2), (zl + 2) % ZN, ZN - 1 - zl][a]


STEPS = [(a, b) for a in (3, 2, 1) for b in (2, 1, 3, 0)] + [(0, b) for b in (2, 1, 3)]


def dot(a, b):
    return jnp.dot(a, b, preferred_element_type=F32)


def dot_t(a, b):
    return lax.dot_general(a, b, (((1,), (1,)), ((), ())), preferred_element_type=F32)


def features(u, omega_pad, kappa, lift, dim_head):
    nfeat = omega_pad[0].shape[-1]
    u32 = u.astype(F32)
    square = u32 * u32 * (-lift) - (0.5 * math.log2(nfeat) / kappa / dim_head)
    high = square.astype(BF16).astype(F32)
    low = pltpu.roll(square - high, dim_head, 1)
    first = lax.broadcasted_iota(jnp.int32, square.shape, 1) < dim_head
    out = []
    for s in range(2):
        parts = jnp.where(first, high, low) if s == 0 else jnp.where(first, low, high)
        lhs = jnp.concatenate([u, parts.astype(BF16)], axis=1)
        arg = dot(lhs, omega_pad[s])
        out.append(jnp.exp2(arg * kappa).astype(BF16))
    return out


def kernel(
    n,
    heads,
    tok_h,
    wq_h,
    wk_h,
    wv_h,
    wo_h,
    om_h,
    ck_h,
    gain_h,
    out,
    tok,
    wq,
    wk,
    wv,
    wo,
    om,
    ck,
    gain,
    omp,
    proj,
    vext,
    halo,
    vt,
    fq,
    pos,
    attn,
    mixed,
    send0,
    recv0,
    send1,
    recv1,
    send2,
    recv2,
    state,
    rhs,
    partial,
    in_sem,
    pair_sem,
    halo_sem,
    rs_sem,
    far_sem,
    ag_sem,
    fw_sem,
    relay_sem,
):
    tokens, width = tok.shape
    cols = halo.shape[1]
    rows_here = tokens // cols
    dim_head = width // heads
    nfeat = om.shape[-1]
    pairs = heads // 2
    lanes = 2 * dim_head
    half = nfeat // 2
    kappa = dim_head ** (-0.25) * math.log2(math.e)
    lift = 0.5 * dim_head ** (-0.5) / dim_head ** (-0.25)

    me = lax.axis_index("row")
    core = me % CORES
    x = (me // CORES) % XS
    z_count = n // (CORES * XS)
    far_count = z_count // ZN
    shift = core * (ZN // 2)
    z = (me // (CORES * XS) + shift) % z_count
    zl, far = z % ZN, z // ZN
    near = slot(zl, x)

    def device(run, zl, x):
        return (((run * ZN + zl + z_count - shift) % z_count) * XS + x) * CORES + core

    partner = me + 1 - 2 * core
    above, below = (me + n - 1) % n, (me + 1) % n
    near_to = [(run_step(zl, a), (x + b) % XS) for a, b in STEPS]
    near_from = [(run_step(zl, a), (x + XS - b) % XS) for a, b in STEPS]
    far_ids = [device((far + d) % far_count, zl, x) for d in range(1, far_count)]
    next_ids = [far_ids[0], far_ids[-1]]

    blocks = [slice(c, c + 256) for c in range(0, width, 256)]

    def load(src, dst, i):
        copy = pltpu.make_async_copy(src, dst, in_sem.at[i])
        copy.start()
        return copy

    tok_load = load(tok_h, tok, 0)
    v_load = load(wv_h, wv, 1)
    k_load = load(wk_h, wk, 2)
    om_load = load(om_h, om, 3)

    barrier = pltpu.get_barrier_semaphore()
    greeted = next_ids + [device(far, *to) for to in near_to] + [above, below, partner]
    for other in greeted:
        pl.semaphore_signal(barrier, inc=1, device_id={"row": other}, device_id_type=MESH)

    for s in range(2):
        for p in range(pairs):
            omp[p, s, (1 - s) * dim_head : (2 - s) * dim_head, :] = jnp.zeros((dim_head, nfeat), BF16)
            omp[p, s, lanes:, :] = jnp.ones((lanes, nfeat), BF16)
    for p in range(pairs):
        vt[p, lanes:, :] = jnp.ones((vt.shape[1] - lanes, tokens), BF16)
    for h in range(2):
        for j in range(NEAR):
            send0[h, j, KV_ROWS:, :] = jnp.zeros((CHUNK - KV_ROWS, half), BF16)

    tok_load.wait()
    v_load.wait()
    for block in blocks:
        vext[cols : cols + tokens, block] = dot(tok[...], wv[:, block]).astype(BF16)
    k_load.wait()
    for block in blocks:
        proj[:, block] = dot(tok[...], wk[:, block]).astype(BF16)
    om_load.wait()
    q_load = load(wq_h, wq, 4)
    ck_load = load(ck_h, ck, 5)
    gain_load = load(gain_h, gain, 6)
    o_load = load(wo_h, wo, 7)
    for p in range(pairs):
        for s in range(2):
            omp[p, s, s * dim_head : (s + 1) * dim_head, :] = om[2 * p + s]
        vt[p, :lanes, :] = vext[cols : cols + tokens, p * lanes : (p + 1) * lanes].T

    def local(own_pairs):
        for p in own_pairs:
            u = proj[:, p * lanes : (p + 1) * lanes]
            feats = features(u, [omp[p, 0], omp[p, 1]], kappa, lift, dim_head)
            for s in range(2):
                head = 2 * p + s
                st = dot(vt[p], feats[s])
                for h in range(2):
                    part = st[:, h * half : (h + 1) * half].astype(BF16)
                    for i in range(dim_head // 16):
                        block = head * (dim_head // 16) + i
                        chunk, place = divmod(block, KV_ROWS // 16)
                        send0[h, chunk, place * 16 : (place + 1) * 16, :] = part[
                            s * dim_head + i * 16 : s * dim_head + (i + 1) * 16
                        ]
                    send0[h, head + head // 3, KV_ROWS:, :] = part[lanes : lanes + CHUNK - KV_ROWS]

    def send(src, dst, sems, recv, other):
        copy = pltpu.make_async_remote_copy(
            src_ref=src,
            dst_ref=dst,
            send_sem=sems.at[0],
            recv_sem=sems.at[recv],
            device_id={"row": other},
            device_id_type=MESH,
        )
        copy.start()

    def wait_sent(ref, sems):
        pltpu.make_async_remote_copy(
            src_ref=ref,
            dst_ref=ref,
            send_sem=sems.at[0],
            recv_sem=sems.at[1],
            device_id={"row": partner},
            device_id_type=MESH,
        ).wait_send()

    def wait_received(ref, sems, recv=1):
        pltpu.make_async_remote_copy(
            src_ref=ref,
            dst_ref=ref,
            send_sem=sems.at[0],
            recv_sem=sems.at[recv],
            device_id={"row": partner},
            device_id_type=MESH,
        ).wait_recv()

    def swap(wave):
        own = pl.ds(wave * ZN, ZN)
        send(send0.at[1 - core, own], recv0.at[own], pair_sem, 1 + wave, partner)

    def scatter(wave):
        for a in (3, 2, 1, 0):
            zp = run_step(zl, a)
            to = (zp, (wave + WAVES - zp) % XS)
            j = slot(*to)
            send1[j] = (send0[core, j].astype(F32) + recv0[j].astype(F32)).astype(BF16)
            start = functools.partial(send, send1.at[j], recv1.at[near], rs_sem, 1, device(far, *to))
            if a == 0:
                pl.when(to[1] != x)(start)
            else:
                start()

    local([0, 1])
    pl.semaphore_wait(barrier, len(greeted))
    for other in next_ids:
        pl.semaphore_signal(relay_sem, inc=1, device_id={"row": other}, device_id_type=MESH)
    swap(0)
    local([2])
    swap(1)
    local([3, 4])
    swap(2)
    wait_received(recv0.at[pl.ds(0, ZN)], pair_sem, 1)
    scatter(0)
    local(range(5, pairs))
    swap(3)
    for wave in range(1, WAVES):
        wait_received(recv0.at[pl.ds(wave * ZN, ZN)], pair_sem, 1 + wave)
        scatter(wave)

    q_load.wait()
    for c in range(0, width, 256):
        proj[:, c : c + 256] = dot(tok[...], wq[:, c : c + 256]).astype(BF16)
    for p in range(pairs):
        u = proj[:, p * lanes : (p + 1) * lanes]
        feats = features(u, [omp[p, 0], omp[p, 1]], kappa, lift, dim_head)
        for s in range(2):
            for h in range(2):
                fq[h, :, (2 * p + s) * half : (2 * p + s + 1) * half] = feats[s][:, h * half : (h + 1) * half]

    wait_received(recv1.at[pl.ds(0, NEAR - 1)], rs_sem)
    recv1[near] = send1[near]
    total = recv1[0].astype(F32)
    for k in range(1, NEAR):
        total = total + recv1[k].astype(F32)
    send2[...] = total.astype(BF16)

    pl.semaphore_wait(relay_sem, len(next_ids))
    for k, other in sorted(enumerate(far_ids), key=lambda item: abs(2 * item[0] + 2 - far_count)):
        send(send2, recv2.at[k], far_sem, 1, other)

    for k, (row, other) in enumerate([(rows_here - 1, below), (0, above)]):
        send(tok.at[pl.ds(row * cols, cols)], halo.at[k], halo_sem, 1, other)

    wait_received(recv2, far_sem)
    total = send2[...].astype(F32)
    for k in range(len(far_ids)):
        total = total + recv2[k].astype(F32)
    state[core, near] = total.astype(BF16)

    for (a, b), to in zip(STEPS, near_to):
        send(state.at[core, near], state.at[core, near], ag_sem, 1 + a, device(far, *to))

    wait_received(halo, halo_sem)
    for k, (edge, place) in enumerate([(0, 0), (n - 1, rows_here + 1)]):
        rows = halo[k]
        rows = jnp.where(me == edge, jnp.zeros_like(rows), rows)
        for c in range(0, width, 256):
            vext[place * cols : (place + 1) * cols, c : c + 256] = dot(rows, wv[:, c : c + 256]).astype(
                BF16
            )
    ck_load.wait()
    column = lax.broadcasted_iota(jnp.int32, (cols, lanes), 0)
    for c in range(0, width, lanes):
        for r in range(rows_here):
            rows = [
                vext[(r + a) * cols : (r + a + 1) * cols, c : c + lanes].astype(F32) for a in range(3)
            ]
            taps = []
            for b in range(3):
                tap = rows[0] * ck[0, b : b + 1, c : c + lanes]
                for a in (1, 2):
                    tap = tap + rows[a] * ck[a, b : b + 1, c : c + lanes]
                taps.append(tap)
            left = jnp.where(column == 0, 0.0, pltpu.roll(taps[0], 1, 0))
            right = jnp.where(column == cols - 1, 0.0, pltpu.roll(taps[2], cols - 1, 0))
            pos[r * cols : (r + 1) * cols, c : c + lanes] = left + taps[1] + right

    def hand_on(j):
        send(state.at[core, j], state.at[core, j], fw_sem, 1, partner)

    hand_on(near)
    for a in range(ZN):
        sources = [source for (step, b), source in zip(STEPS, near_from) if step == a]
        wait_received(state.at[core, pl.ds(0, len(sources))], ag_sem, 1 + a)
        for source in sources:
            hand_on(slot(*source))

    blank = jnp.zeros((dim_head, half), BF16)

    def operand(slot, h):
        for p in range(pairs):
            parts, sums = [], []
            for s in range(2):
                head = 2 * p + s
                tiles = []
                for i in range(dim_head // 16):
                    chunk, place = divmod(head * (dim_head // 16) + i, KV_ROWS // 16)
                    tiles.append(state[h, chunk, place * 16 : (place + 1) * 16, :])
                parts.append(jnp.concatenate(tiles, axis=0))
                key_sum = state[h, head + head // 3, KV_ROWS:, :]
                sums.append(jnp.concatenate([key_sum] * (dim_head // (CHUNK - KV_ROWS)), axis=0))
            for s in range(2):
                for i, block in enumerate([parts, sums]):
                    for t in range(2):
                        rhs[slot, p, (2 * i + t) * dim_head : (2 * i + t + 1) * dim_head, s * half : (s + 1) * half] = (
                            block[s] if s == t else blank
                        )

    operand(0, core)
    for p in range(pairs):
        at = slice(p * 2 * lanes, (p + 1) * 2 * lanes)
        partial[:, at] = dot_t(fq[core, :, at], rhs[0, p])
    wait_received(state.at[1 - core], fw_sem)
    wait_sent(send0.at[1 - core], pair_sem)
    wait_sent(send1.at[pl.ds(0, NEAR - 1)], rs_sem)
    wait_sent(recv2, far_sem)
    wait_sent(halo, halo_sem)
    wait_sent(state.at[core, pl.ds(0, NEAR - 1)], ag_sem)
    wait_sent(state.at[core], fw_sem)
    operand(1, 1 - core)
    gain_load.wait()
    o_load.wait()
    for p in range(pairs):
        on = slice(p * 2 * lanes, (p + 1) * 2 * lanes)
        both = partial[:, on] + dot_t(fq[1 - core, :, on], rhs[1, p])
        attn[:, p * lanes : (p + 1) * lanes] = both[:, :lanes] / both[:, lanes:]
    for r in range(rows_here):
        at = slice(r * cols, (r + 1) * cols)
        squares = jnp.zeros((cols, lanes), F32)
        for c in range(0, width, lanes):
            ratio = attn[at, c : c + lanes]
            squares = squares + ratio * ratio
        scale = lax.rsqrt(jnp.sum(squares, axis=1, keepdims=True) * (1.0 / width) + 1e-06)
        for c in range(0, width, lanes):
            normed = attn[at, c : c + lanes] * scale * gain[c : c + lanes].reshape(1, lanes)
            mixed[at, c : c + lanes] = (normed + pos[at, c : c + lanes]).astype(BF16)
        for c in range(0, width, 256):
            out[at, c : c + 256] = (
                tok[at, c : c + 256].astype(F32) + dot(mixed[at], wo[:, c : c + 256])
            ).astype(BF16)


def layer(n, tokens, w_query, w_key, w_value, w_out, omega, conv_kernel, norm_gain):
    rows_here, cols, width = tokens.shape
    heads, dim_head, nfeat = omega.shape
    count = rows_here * cols
    pairs, lanes, half = heads // 2, 2 * dim_head, nfeat // 2
    far = n // (CORES * NEAR) - 1
    steps = len(STEPS)
    vmem = pltpu.VMEM
    dma = pltpu.SemaphoreType.DMA
    out = pl.pallas_call(
        functools.partial(kernel, n, heads),
        out_shape=jax.ShapeDtypeStruct((count, width), BF16),
        in_specs=[pl.BlockSpec(memory_space=pl.ANY)] * 8,
        out_specs=pl.BlockSpec(memory_space=pltpu.VMEM),
        scratch_shapes=[
            vmem((count, width), BF16),
            vmem((width, width), BF16),
            vmem((width, width), BF16),
            vmem((width, width), BF16),
            vmem((width, width), BF16),
            vmem((heads, dim_head, nfeat), BF16),
            vmem((3, 3, width), F32),
            vmem((width,), F32),
            vmem((pairs, 2, 2 * lanes, nfeat), BF16),
            vmem((count, width), BF16),
            vmem((count + 2 * cols, width), BF16),
            vmem((2, cols, width), BF16),
            vmem((pairs, lanes + 16, count), BF16),
            vmem((2, count, heads * half), BF16),
            vmem((count, width), F32),
            vmem((count, width), F32),
            vmem((count, width), BF16),
            vmem((2, NEAR, CHUNK, half), BF16),
            vmem((NEAR, CHUNK, half), BF16),
            vmem((NEAR, CHUNK, half), BF16),
            vmem((NEAR, CHUNK, half), BF16),
            vmem((CHUNK, half), BF16),
            vmem((far, CHUNK, half), BF16),
            vmem((2, NEAR, CHUNK, half), BF16),
            vmem((2, pairs, 2 * lanes, nfeat), BF16),
            vmem((count, pairs * 2 * lanes), F32),
            dma((8,)),
            dma((1 + WAVES,)),
            dma((2,)),
            dma((2,)),
            dma((2,)),
            dma((1 + ZN,)),
            dma((2,)),
            pltpu.SemaphoreType.REGULAR,
        ],
        compiler_params=pltpu.CompilerParams(
            collective_id=0, has_side_effects=True, vmem_limit_bytes=48 * 1024 * 1024
        ),
        name="favor_layer",
    )(
        *[
            pltpu.with_memory_space_constraint(operand, pltpu.HBM)
            for operand in (
                tokens.reshape(count, width),
                w_query,
                w_key,
                w_value,
                w_out,
                omega,
                conv_kernel,
                norm_gain,
            )
        ]
    )
    return out.reshape(rows_here, cols, width)


def solution(mesh):
    return jax.shard_map(
        functools.partial(layer, mesh.shape["row"]),
        mesh=mesh,
        in_specs=(P(("parts", "row"), None, None), P(), P(), P(), P(), P(), P(), P()),
        out_specs=P(("parts", "row"), None, None),
        check_vma=False,
    )
```

```python
import functools
import math

import jax
import jax.numpy as jnp
from jax import lax
from jax.experimental import pallas as pl
from jax.experimental.pallas import tpu as pltpu
from jax.sharding import PartitionSpec as P

MESH = pl.DeviceIdType.MESH
F32 = jnp.float32
BF16 = jnp.bfloat16

XS = 4
ZN = 4
CORES = 2
NEAR = XS * ZN
WAVES = XS
KV_ROWS = 48
CHUNK = 56


def slot(zl, x):
    return (zl + x) % WAVES * ZN + zl


def run_step(zl, a):
    return [zl, zl + 1 - 2 * (zl % 2), (zl + 2) % ZN, ZN - 1 - zl][a]


STEPS = [(a, b) for a in (3, 2, 1) for b in (2, 1, 3, 0)] + [(0, b) for b in (2, 1, 3)]


def dot(a, b):
    return jnp.dot(a, b, preferred_element_type=F32)


def dot_t(a, b):
    return lax.dot_general(a, b, (((1,), (1,)), ((), ())), preferred_element_type=F32)


def features(u, omega_pad, kappa, lift, dim_head):
    nfeat = omega_pad[0].shape[-1]
    u32 = u.astype(F32)
    square = u32 * u32 * (-lift) - (0.5 * math.log2(nfeat) / kappa / dim_head)
    high = square.astype(BF16).astype(F32)
    low = pltpu.roll(square - high, dim_head, 1)
    first = lax.broadcasted_iota(jnp.int32, square.shape, 1) < dim_head
    out = []
    for s in range(2):
        parts = jnp.where(first, high, low) if s == 0 else jnp.where(first, low, high)
        lhs = jnp.concatenate([u, parts.astype(BF16)], axis=1)
        arg = dot(lhs, omega_pad[s])
        out.append(jnp.exp2(arg * kappa).astype(BF16))
    return out


def kernel(
    n,
    heads,
    tok_h,
    wq_h,
    wk_h,
    wv_h,
    wo_h,
    om_h,
    ck_h,
    gain_h,
    out,
    tok,
    wq,
    wk,
    wv,
    wo,
    om,
    ck,
    gain,
    omp,
    proj,
    vext,
    halo,
    vt,
    fq,
    pos,
    attn,
    mixed,
    send0,
    recv0,
    send1,
    recv1,
    send2,
    recv2,
    state,
    rhs,
    partial,
    in_sem,
    pair_sem,
    halo_sem,
    rs_sem,
    far_sem,
    ag_sem,
    fw_sem,
    relay_sem,
):
    tokens, width = tok.shape
    cols = halo.shape[1]
    rows_here = tokens // cols
    dim_head = width // heads
    nfeat = om.shape[-1]
    pairs = heads // 2
    lanes = 2 * dim_head
    half = nfeat // 2
    kappa = dim_head ** (-0.25) * math.log2(math.e)
    lift = 0.5 * dim_head ** (-0.5) / dim_head ** (-0.25)

    blocks = [slice(c, c + 256) for c in range(0, width, 256)]

    def load(src, dst, i):
        copy = pltpu.make_async_copy(src, dst, in_sem.at[i])
        copy.start()
        return copy

    tok_load = load(tok_h, tok, 0)
    v_load = load(wv_h, wv, 1)
    k_load = load(wk_h, wk, 2)
    om_load = load(om_h, om, 3)

    me = lax.axis_index("row")
    core = me % CORES
    x = (me // CORES) % XS
    z_count = n // (CORES * XS)
    far_count = z_count // ZN
    shift = core * (ZN // 2)
    z = (me // (CORES * XS) + shift) % z_count
    zl, far = z % ZN, z // ZN
    near = slot(zl, x)

    def device(run, zl, x):
        return (((run * ZN + zl + z_count - shift) % z_count) * XS + x) * CORES + core

    partner = me + 1 - 2 * core
    above, below = (me + n - 1) % n, (me + 1) % n
    near_to = [(run_step(zl, a), (x + b) % XS) for a, b in STEPS]
    near_from = [(run_step(zl, a), (x + XS - b) % XS) for a, b in STEPS]
    far_ids = [device((far + d) % far_count, zl, x) for d in range(1, far_count)]
    next_ids = [far_ids[0], far_ids[-1]]

    barrier = pltpu.get_barrier_semaphore()
    greeted = [device(far, *to) for to in near_to] + [above, below, partner]

    def tell_runs(sem):
        for end, other in zip((far_count - 2, far_count - 1), next_ids):

            @pl.when(far != end)
            def _(other=other):
                pl.semaphore_signal(sem, inc=1, device_id={"row": other}, device_id_type=MESH)

    tell_runs(barrier)
    for other in greeted:
        pl.semaphore_signal(barrier, inc=1, device_id={"row": other}, device_id_type=MESH)

    for s in range(2):
        for p in range(pairs):
            omp[p, s, (1 - s) * dim_head : (2 - s) * dim_head, :] = jnp.zeros((dim_head, nfeat), BF16)
            omp[p, s, lanes:, :] = jnp.ones((lanes, nfeat), BF16)
    for p in range(pairs):
        vt[p, lanes:, :] = jnp.ones((vt.shape[1] - lanes, tokens), BF16)
    for h in range(2):
        for j in range(NEAR):
            send0[h, j, KV_ROWS:, :] = jnp.zeros((CHUNK - KV_ROWS, half), BF16)

    tok_load.wait()
    v_load.wait()
    for block in blocks:
        vext[cols : cols + tokens, block] = dot(tok[...], wv[:, block]).astype(BF16)
    k_load.wait()
    for block in blocks:
        proj[:, block] = dot(tok[...], wk[:, block]).astype(BF16)
    om_load.wait()
    q_load = load(wq_h, wq, 4)
    ck_load = load(ck_h, ck, 5)
    gain_load = load(gain_h, gain, 6)
    o_load = load(wo_h, wo, 7)
    for p in range(pairs):
        for s in range(2):
            omp[p, s, s * dim_head : (s + 1) * dim_head, :] = om[2 * p + s]
        vt[p, :lanes, :] = vext[cols : cols + tokens, p * lanes : (p + 1) * lanes].T

    def local(own_pairs):
        for p in own_pairs:
            u = proj[:, p * lanes : (p + 1) * lanes]
            feats = features(u, [omp[p, 0], omp[p, 1]], kappa, lift, dim_head)
            for s in range(2):
                head = 2 * p + s
                st = dot(vt[p], feats[s])
                for h in range(2):
                    part = st[:, h * half : (h + 1) * half].astype(BF16)
                    for i in range(dim_head // 16):
                        block = head * (dim_head // 16) + i
                        chunk, place = divmod(block, KV_ROWS // 16)
                        send0[h, chunk, place * 16 : (place + 1) * 16, :] = part[
                            s * dim_head + i * 16 : s * dim_head + (i + 1) * 16
                        ]
                    send0[h, head + head // 3, KV_ROWS:, :] = part[lanes : lanes + CHUNK - KV_ROWS]

    def send(src, dst, sems, recv, other):
        copy = pltpu.make_async_remote_copy(
            src_ref=src,
            dst_ref=dst,
            send_sem=sems.at[0],
            recv_sem=sems.at[recv],
            device_id={"row": other},
            device_id_type=MESH,
        )
        copy.start()

    def wait_sent(ref, sems):
        pltpu.make_async_remote_copy(
            src_ref=ref,
            dst_ref=ref,
            send_sem=sems.at[0],
            recv_sem=sems.at[1],
            device_id={"row": partner},
            device_id_type=MESH,
        ).wait_send()

    def wait_received(ref, sems, recv=1):
        pltpu.make_async_remote_copy(
            src_ref=ref,
            dst_ref=ref,
            send_sem=sems.at[0],
            recv_sem=sems.at[recv],
            device_id={"row": partner},
            device_id_type=MESH,
        ).wait_recv()

    def swap(wave):
        own = pl.ds(wave * ZN, ZN)
        send(send0.at[1 - core, own], recv0.at[own], pair_sem, 1 + wave, partner)

    def scatter(wave):
        for a in (3, 2, 1, 0):
            zp = run_step(zl, a)
            to = (zp, (wave + WAVES - zp) % XS)
            j = slot(*to)
            send1[j] = (send0[core, j].astype(F32) + recv0[j].astype(F32)).astype(BF16)
            start = functools.partial(send, send1.at[j], recv1.at[near], rs_sem, 1, device(far, *to))
            if a == 0:
                pl.when(to[1] != x)(start)
            else:
                start()

    local([0, 1])
    pl.semaphore_wait(barrier, len(greeted) + 2 - far // (far_count // 2))
    tell_runs(relay_sem)
    swap(0)
    local([2])
    swap(1)
    local([3, 4])
    swap(2)
    wait_received(recv0.at[pl.ds(0, ZN)], pair_sem, 1)
    scatter(0)
    local(range(5, pairs))
    swap(3)
    for wave in range(1, WAVES):
        wait_received(recv0.at[pl.ds(wave * ZN, ZN)], pair_sem, 1 + wave)
        scatter(wave)

    q_load.wait()
    for c in range(0, width, 256):
        proj[:, c : c + 256] = dot(tok[...], wq[:, c : c + 256]).astype(BF16)
    for p in range(pairs):
        u = proj[:, p * lanes : (p + 1) * lanes]
        feats = features(u, [omp[p, 0], omp[p, 1]], kappa, lift, dim_head)
        for s in range(2):
            for h in range(2):
                fq[h, :, (2 * p + s) * half : (2 * p + s + 1) * half] = feats[s][:, h * half : (h + 1) * half]

    line = CORES * XS

    def halo_rows(crossing):
        for k, (row, other, end) in enumerate([(rows_here - 1, below, line - 1), (0, above, 0)]):
            start = functools.partial(
                send, tok.at[pl.ds(row * cols, cols)], halo.at[k], halo_sem, 1, other
            )
            pl.when(me % line == end if crossing else me % line != end)(start)

    halo_rows(False)

    @pl.when(far < far_count // 2)
    def _():
        pl.semaphore_wait(relay_sem, 2)
        end = jnp.where(far == 0, next_ids[1], next_ids[0])
        pl.semaphore_signal(relay_sem, inc=1, device_id={"row": end}, device_id_type=MESH)

    wait_received(recv1.at[pl.ds(0, NEAR - 1)], rs_sem)
    recv1[near] = send1[near]
    total = recv1[0].astype(F32)
    for k in range(1, NEAR):
        total = total + recv1[k].astype(F32)
    send2[...] = total.astype(BF16)


    @pl.when(far >= far_count // 2)
    def _():
        pl.semaphore_wait(relay_sem, 2)

    for k, other in sorted(enumerate(far_ids), key=lambda item: abs(2 * item[0] + 2 - far_count)):
        send(send2, recv2.at[k], far_sem, 1, other)

    halo_rows(True)

    wait_received(recv2, far_sem)
    total = send2[...].astype(F32)
    for k in range(len(far_ids)):
        total = total + recv2[k].astype(F32)
    state[core, near] = total.astype(BF16)

    for (a, b), to in zip(STEPS, near_to):
        send(state.at[core, near], state.at[core, near], ag_sem, 1 + a, device(far, *to))

    wait_received(halo, halo_sem)
    for k, (edge, place) in enumerate([(0, 0), (n - 1, rows_here + 1)]):
        rows = halo[k]
        rows = jnp.where(me == edge, jnp.zeros_like(rows), rows)
        for c in range(0, width, 256):
            vext[place * cols : (place + 1) * cols, c : c + 256] = dot(rows, wv[:, c : c + 256]).astype(
                BF16
            )
    ck_load.wait()
    column = lax.broadcasted_iota(jnp.int32, (cols, lanes), 0)
    for c in range(0, width, lanes):
        for r in range(rows_here):
            rows = [
                vext[(r + a) * cols : (r + a + 1) * cols, c : c + lanes].astype(F32) for a in range(3)
            ]
            taps = []
            for b in range(3):
                tap = rows[0] * ck[0, b : b + 1, c : c + lanes]
                for a in (1, 2):
                    tap = tap + rows[a] * ck[a, b : b + 1, c : c + lanes]
                taps.append(tap)
            left = jnp.where(column == 0, 0.0, pltpu.roll(taps[0], 1, 0))
            right = jnp.where(column == cols - 1, 0.0, pltpu.roll(taps[2], cols - 1, 0))
            pos[r * cols : (r + 1) * cols, c : c + lanes] = left + taps[1] + right

    def hand_on(j):
        send(state.at[core, j], state.at[core, j], fw_sem, 1, partner)

    hand_on(near)
    for a in range(ZN):
        sources = [source for (step, b), source in zip(STEPS, near_from) if step == a]
        wait_received(state.at[core, pl.ds(0, len(sources))], ag_sem, 1 + a)
        for source in sources:
            hand_on(slot(*source))

    blank = jnp.zeros((dim_head, half), BF16)

    def operand(slot, h):
        for p in range(pairs):
            parts, sums = [], []
            for s in range(2):
                head = 2 * p + s
                tiles = []
                for i in range(dim_head // 16):
                    chunk, place = divmod(head * (dim_head // 16) + i, KV_ROWS // 16)
                    tiles.append(state[h, chunk, place * 16 : (place + 1) * 16, :])
                parts.append(jnp.concatenate(tiles, axis=0))
                key_sum = state[h, head + head // 3, KV_ROWS:, :]
                sums.append(jnp.concatenate([key_sum] * (dim_head // (CHUNK - KV_ROWS)), axis=0))
            for s in range(2):
                for i, block in enumerate([parts, sums]):
                    for t in range(2):
                        rhs[slot, p, (2 * i + t) * dim_head : (2 * i + t + 1) * dim_head, s * half : (s + 1) * half] = (
                            block[s] if s == t else blank
                        )

    operand(0, core)
    for p in range(pairs):
        at = slice(p * 2 * lanes, (p + 1) * 2 * lanes)
        partial[:, at] = dot_t(fq[core, :, at], rhs[0, p])
    wait_received(state.at[1 - core], fw_sem)
    wait_sent(send0.at[1 - core], pair_sem)
    wait_sent(send1.at[pl.ds(0, NEAR - 1)], rs_sem)
    wait_sent(recv2, far_sem)
    wait_sent(halo, halo_sem)
    wait_sent(state.at[core, pl.ds(0, NEAR - 1)], ag_sem)
    wait_sent(state.at[core], fw_sem)
    operand(1, 1 - core)
    gain_load.wait()
    o_load.wait()
    for p in range(pairs):
        on = slice(p * 2 * lanes, (p + 1) * 2 * lanes)
        both = partial[:, on] + dot_t(fq[1 - core, :, on], rhs[1, p])
        attn[:, p * lanes : (p + 1) * lanes] = both[:, :lanes] / both[:, lanes:]
    for r in range(rows_here):
        at = slice(r * cols, (r + 1) * cols)
        squares = jnp.zeros((cols, lanes), F32)
        for c in range(0, width, lanes):
            ratio = attn[at, c : c + lanes]
            squares = squares + ratio * ratio
        scale = lax.rsqrt(jnp.sum(squares, axis=1, keepdims=True) * (1.0 / width) + 1e-06)
        for c in range(0, width, lanes):
            normed = attn[at, c : c + lanes] * scale * gain[c : c + lanes].reshape(1, lanes)
            mixed[at, c : c + lanes] = (normed + pos[at, c : c + lanes]).astype(BF16)
        for c in range(0, width, 256):
            out[at, c : c + 256] = (
                tok[at, c : c + 256].astype(F32) + dot(mixed[at], wo[:, c : c + 256])
            ).astype(BF16)


def layer(n, tokens, w_query, w_key, w_value, w_out, omega, conv_kernel, norm_gain):
    rows_here, cols, width = tokens.shape
    heads, dim_head, nfeat = omega.shape
    count = rows_here * cols
    pairs, lanes, half = heads // 2, 2 * dim_head, nfeat // 2
    far = n // (CORES * NEAR) - 1
    steps = len(STEPS)
    vmem = pltpu.VMEM
    dma = pltpu.SemaphoreType.DMA
    out = pl.pallas_call(
        functools.partial(kernel, n, heads),
        out_shape=jax.ShapeDtypeStruct((count, width), BF16),
        in_specs=[pl.BlockSpec(memory_space=pl.ANY)] * 8,
        out_specs=pl.BlockSpec(memory_space=pltpu.VMEM),
        scratch_shapes=[
            vmem((count, width), BF16),
            vmem((width, width), BF16),
            vmem((width, width), BF16),
            vmem((width, width), BF16),
            vmem((width, width), BF16),
            vmem((heads, dim_head, nfeat), BF16),
            vmem((3, 3, width), F32),
            vmem((width,), F32),
            vmem((pairs, 2, 2 * lanes, nfeat), BF16),
            vmem((count, width), BF16),
            vmem((count + 2 * cols, width), BF16),
            vmem((2, cols, width), BF16),
            vmem((pairs, lanes + 16, count), BF16),
            vmem((2, count, heads * half), BF16),
            vmem((count, width), F32),
            vmem((count, width), F32),
            vmem((count, width), BF16),
            vmem((2, NEAR, CHUNK, half), BF16),
            vmem((NEAR, CHUNK, half), BF16),
            vmem((NEAR, CHUNK, half), BF16),
            vmem((NEAR, CHUNK, half), BF16),
            vmem((CHUNK, half), BF16),
            vmem((far, CHUNK, half), BF16),
            vmem((2, NEAR, CHUNK, half), BF16),
            vmem((2, pairs, 2 * lanes, nfeat), BF16),
            vmem((count, pairs * 2 * lanes), F32),
            dma((8,)),
            dma((1 + WAVES,)),
            dma((2,)),
            dma((2,)),
            dma((2,)),
            dma((1 + ZN,)),
            dma((2,)),
            pltpu.SemaphoreType.REGULAR,
        ],
        compiler_params=pltpu.CompilerParams(
            collective_id=0, has_side_effects=True, vmem_limit_bytes=48 * 1024 * 1024
        ),
        name="favor_layer",
    )(
        *[
            pltpu.with_memory_space_constraint(operand, pltpu.HBM)
            for operand in (
                tokens.reshape(count, width),
                w_query,
                w_key,
                w_value,
                w_out,
                omega,
                conv_kernel,
                norm_gain,
            )
        ]
    )
    return out.reshape(rows_here, cols, width)


def solution(mesh):
    return jax.shard_map(
        functools.partial(layer, mesh.shape["row"]),
        mesh=mesh,
        in_specs=(P(("parts", "row"), None, None), P(), P(), P(), P(), P(), P(), P()),
        out_specs=P(("parts", "row"), None, None),
        check_vma=False,
    )
```

```python
import functools
import math

import jax
import jax.numpy as jnp
from jax import lax
from jax.experimental import pallas as pl
from jax.experimental.pallas import tpu as pltpu
from jax.sharding import PartitionSpec as P

MESH = pl.DeviceIdType.MESH
F32 = jnp.float32
BF16 = jnp.bfloat16

XS = 4
ZN = 4
CORES = 2
NEAR = XS * ZN
WAVES = XS
KV_ROWS = 48
CHUNK = 56


def slot(zl, x):
    return (zl + x) % WAVES * ZN + zl


def run_step(zl, a):
    return [zl, zl + 1 - 2 * (zl % 2), (zl + 2) % ZN, ZN - 1 - zl][a]


STEPS = [(a, b) for a in (3, 2, 1) for b in (2, 1, 3, 0)] + [(0, b) for b in (2, 1, 3)]


def dot(a, b):
    return jnp.dot(a, b, preferred_element_type=F32)


def dot_t(a, b):
    return lax.dot_general(a, b, (((1,), (1,)), ((), ())), preferred_element_type=F32)


def features(u, omega_pad, kappa, lift, dim_head):
    nfeat = omega_pad[0].shape[-1]
    u32 = u.astype(F32)
    square = u32 * u32 * (-lift) - (0.5 * math.log2(nfeat) / kappa / dim_head)
    high = square.astype(BF16).astype(F32)
    low = pltpu.roll(square - high, dim_head, 1)
    first = lax.broadcasted_iota(jnp.int32, square.shape, 1) < dim_head
    out = []
    for s in range(2):
        parts = jnp.where(first, high, low) if s == 0 else jnp.where(first, low, high)
        lhs = jnp.concatenate([u, parts.astype(BF16)], axis=1)
        arg = dot(lhs, omega_pad[s])
        out.append(jnp.exp2(arg * kappa).astype(BF16))
    return out


def kernel(
    n,
    heads,
    tok_h,
    wq_h,
    wk_h,
    wv_h,
    wo_h,
    om_h,
    ck_h,
    gain_h,
    out,
    tok,
    wq,
    wk,
    wv,
    wo,
    om,
    ck,
    gain,
    omp,
    proj,
    vext,
    halo,
    vt,
    fq,
    pos,
    attn,
    mixed,
    send0,
    recv0,
    send1,
    recv1,
    send2,
    recv2,
    state,
    rhs,
    partial,
    in_sem,
    pair_sem,
    halo_sem,
    rs_sem,
    far_sem,
    ag_sem,
    fw_sem,
    relay_sem,
):
    tokens, width = tok.shape
    cols = halo.shape[1]
    rows_here = tokens // cols
    dim_head = width // heads
    nfeat = om.shape[-1]
    pairs = heads // 2
    lanes = 2 * dim_head
    half = nfeat // 2
    kappa = dim_head ** (-0.25) * math.log2(math.e)
    lift = 0.5 * dim_head ** (-0.5) / dim_head ** (-0.25)

    blocks = [slice(c, c + 256) for c in range(0, width, 256)]

    def load(src, dst, i):
        copy = pltpu.make_async_copy(src, dst, in_sem.at[i])
        copy.start()
        return copy

    tok_load = load(tok_h, tok, 0)
    v_load = load(wv_h, wv, 1)
    k_load = load(wk_h, wk, 2)
    om_load = load(om_h, om, 3)

    me = lax.axis_index("row")
    core = me % CORES
    x = (me // CORES) % XS
    z_count = n // (CORES * XS)
    far_count = z_count // ZN
    shift = core * (ZN // 2)
    z = (me // (CORES * XS) + shift) % z_count
    zl, far = z % ZN, z // ZN
    near = slot(zl, x)

    def device(run, zl, x):
        return (((run * ZN + zl + z_count - shift) % z_count) * XS + x) * CORES + core

    partner = me + 1 - 2 * core
    above, below = (me + n - 1) % n, (me + 1) % n
    near_to = [(run_step(zl, a), (x + b) % XS) for a, b in STEPS]
    near_from = [(run_step(zl, a), (x + XS - b) % XS) for a, b in STEPS]
    far_ids = [device((far + d) % far_count, zl, x) for d in range(1, far_count)]
    next_ids = [far_ids[0], far_ids[-1]]

    barrier = pltpu.get_barrier_semaphore()
    greeted = [device(far, *to) for to in near_to] + [above, below, partner]

    def tell_runs(sem):
        for end, other in zip((far_count - 2, far_count - 1), next_ids):

            @pl.when(far != end)
            def _(other=other):
                pl.semaphore_signal(sem, inc=1, device_id={"row": other}, device_id_type=MESH)

    tell_runs(barrier)
    for other in greeted:
        pl.semaphore_signal(barrier, inc=1, device_id={"row": other}, device_id_type=MESH)

    for s in range(2):
        for p in range(pairs):
            omp[p, s, (1 - s) * dim_head : (2 - s) * dim_head, :] = jnp.zeros((dim_head, nfeat), BF16)
            omp[p, s, lanes:, :] = jnp.ones((lanes, nfeat), BF16)
    for p in range(pairs):
        vt[p, lanes:, :] = jnp.ones((vt.shape[1] - lanes, tokens), BF16)
    for h in range(2):
        for j in range(NEAR):
            send0[h, j, KV_ROWS:, :] = jnp.zeros((CHUNK - KV_ROWS, half), BF16)

    tok_load.wait()
    v_load.wait()
    for block in blocks:
        vext[cols : cols + tokens, block] = dot(tok[...], wv[:, block]).astype(BF16)
    k_load.wait()
    for block in blocks:
        proj[:, block] = dot(tok[...], wk[:, block]).astype(BF16)
    om_load.wait()
    q_load = load(wq_h, wq, 4)
    ck_load = load(ck_h, ck, 5)
    gain_load = load(gain_h, gain, 6)
    o_load = load(wo_h, wo, 7)
    for p in range(pairs):
        for s in range(2):
            omp[p, s, s * dim_head : (s + 1) * dim_head, :] = om[2 * p + s]
        vt[p, :lanes, :] = vext[cols : cols + tokens, p * lanes : (p + 1) * lanes].T

    def local(own_pairs):
        for p in own_pairs:
            u = proj[:, p * lanes : (p + 1) * lanes]
            feats = features(u, [omp[p, 0], omp[p, 1]], kappa, lift, dim_head)
            for s in range(2):
                head = 2 * p + s
                st = dot(vt[p], feats[s])
                for h in range(2):
                    part = st[:, h * half : (h + 1) * half].astype(BF16)
                    for i in range(dim_head // 16):
                        block = head * (dim_head // 16) + i
                        chunk, place = divmod(block, KV_ROWS // 16)
                        send0[h, chunk, place * 16 : (place + 1) * 16, :] = part[
                            s * dim_head + i * 16 : s * dim_head + (i + 1) * 16
                        ]
                    send0[h, head + head // 3, KV_ROWS:, :] = part[lanes : lanes + CHUNK - KV_ROWS]

    def send(src, dst, sems, recv, other):
        copy = pltpu.make_async_remote_copy(
            src_ref=src,
            dst_ref=dst,
            send_sem=sems.at[0],
            recv_sem=sems.at[recv],
            device_id={"row": other},
            device_id_type=MESH,
        )
        copy.start()

    def wait_sent(ref, sems):
        pltpu.make_async_remote_copy(
            src_ref=ref,
            dst_ref=ref,
            send_sem=sems.at[0],
            recv_sem=sems.at[1],
            device_id={"row": partner},
            device_id_type=MESH,
        ).wait_send()

    def wait_received(ref, sems, recv=1):
        pltpu.make_async_remote_copy(
            src_ref=ref,
            dst_ref=ref,
            send_sem=sems.at[0],
            recv_sem=sems.at[recv],
            device_id={"row": partner},
            device_id_type=MESH,
        ).wait_recv()

    def swap(wave):
        own = pl.ds(wave * ZN, ZN)
        send(send0.at[1 - core, own], recv0.at[own], pair_sem, 1 + wave, partner)

    def scatter(wave):
        for a in (3, 2, 1, 0):
            zp = run_step(zl, a)
            to = (zp, (wave + WAVES - zp) % XS)
            j = slot(*to)
            send1[j] = (send0[core, j].astype(F32) + recv0[j].astype(F32)).astype(BF16)
            start = functools.partial(send, send1.at[j], recv1.at[near], rs_sem, 1, device(far, *to))
            if a == 0:
                pl.when(to[1] != x)(start)
            else:
                start()

    local([0, 1])
    pl.semaphore_wait(barrier, len(greeted) + 2 - far // (far_count // 2))
    tell_runs(relay_sem)
    swap(0)
    local([2])
    swap(1)
    local([3, 4])
    swap(2)
    wait_received(recv0.at[pl.ds(0, ZN)], pair_sem, 1)
    scatter(0)
    local(range(5, pairs))
    swap(3)
    for wave in range(1, WAVES):
        wait_received(recv0.at[pl.ds(wave * ZN, ZN)], pair_sem, 1 + wave)
        scatter(wave)

    q_load.wait()
    for c in range(0, width, 256):
        proj[:, c : c + 256] = dot(tok[...], wq[:, c : c + 256]).astype(BF16)
    for p in range(pairs):
        u = proj[:, p * lanes : (p + 1) * lanes]
        feats = features(u, [omp[p, 0], omp[p, 1]], kappa, lift, dim_head)
        for s in range(2):
            for h in range(2):
                fq[h, :, (2 * p + s) * half : (2 * p + s + 1) * half] = feats[s][:, h * half : (h + 1) * half]

    line = CORES * XS

    def halo_rows(crossing):
        for k, (row, other, end) in enumerate([(rows_here - 1, below, line - 1), (0, above, 0)]):
            start = functools.partial(
                send, tok.at[pl.ds(row * cols, cols)], halo.at[k], halo_sem, 1, other
            )
            pl.when(me % line == end if crossing else me % line != end)(start)

    halo_rows(False)

    @pl.when(far < far_count // 2)
    def _():
        pl.semaphore_wait(relay_sem, 2)
        end = jnp.where(far == 0, next_ids[1], next_ids[0])
        pl.semaphore_signal(relay_sem, inc=1, device_id={"row": end}, device_id_type=MESH)

    for half_of in range(2):
        for p in range(pairs):
            for i in range(2):
                for s in range(2):
                    rows = slice((2 * i + 1 - s) * dim_head, (2 * i + 2 - s) * dim_head)
                    rhs[half_of, p, rows, s * half : (s + 1) * half] = jnp.zeros((dim_head, half), BF16)

    wait_received(recv1.at[pl.ds(0, NEAR - 1)], rs_sem)
    recv1[near] = send1[near]
    total = recv1[0].astype(F32)
    for k in range(1, NEAR):
        total = total + recv1[k].astype(F32)
    send2[...] = total.astype(BF16)


    @pl.when(far >= far_count // 2)
    def _():
        pl.semaphore_wait(relay_sem, 2)

    for k, other in sorted(enumerate(far_ids), key=lambda item: abs(2 * item[0] + 2 - far_count)):
        send(send2, recv2.at[k], far_sem, 1, other)

    halo_rows(True)

    wait_received(recv2, far_sem)
    total = send2[...].astype(F32)
    for k in range(len(far_ids)):
        total = total + recv2[k].astype(F32)
    state[core, near] = total.astype(BF16)

    for (a, b), to in zip(STEPS, near_to):
        send(state.at[core, near], state.at[core, near], ag_sem, 1 + a, device(far, *to))

    wait_received(halo, halo_sem)
    for k, (edge, place) in enumerate([(0, 0), (n - 1, rows_here + 1)]):
        rows = halo[k]
        rows = jnp.where(me == edge, jnp.zeros_like(rows), rows)
        for c in range(0, width, 256):
            vext[place * cols : (place + 1) * cols, c : c + 256] = dot(rows, wv[:, c : c + 256]).astype(
                BF16
            )
    ck_load.wait()
    column = lax.broadcasted_iota(jnp.int32, (cols, lanes), 0)
    for c in range(0, width, lanes):
        for r in range(rows_here):
            rows = [
                vext[(r + a) * cols : (r + a + 1) * cols, c : c + lanes].astype(F32) for a in range(3)
            ]
            taps = []
            for b in range(3):
                tap = rows[0] * ck[0, b : b + 1, c : c + lanes]
                for a in (1, 2):
                    tap = tap + rows[a] * ck[a, b : b + 1, c : c + lanes]
                taps.append(tap)
            left = jnp.where(column == 0, 0.0, pltpu.roll(taps[0], 1, 0))
            right = jnp.where(column == cols - 1, 0.0, pltpu.roll(taps[2], cols - 1, 0))
            pos[r * cols : (r + 1) * cols, c : c + lanes] = left + taps[1] + right

    def hand_on(j):
        send(state.at[core, j], state.at[core, j], fw_sem, 1, partner)

    hand_on(near)
    for a in range(ZN):
        sources = [source for (step, b), source in zip(STEPS, near_from) if step == a]
        wait_received(state.at[core, pl.ds(0, len(sources))], ag_sem, 1 + a)
        for source in sources:
            hand_on(slot(*source))


    def operand(slot, h):
        for p in range(pairs):
            parts, sums = [], []
            for s in range(2):
                head = 2 * p + s
                tiles = []
                for i in range(dim_head // 16):
                    chunk, place = divmod(head * (dim_head // 16) + i, KV_ROWS // 16)
                    tiles.append(state[h, chunk, place * 16 : (place + 1) * 16, :])
                parts.append(jnp.concatenate(tiles, axis=0))
                key_sum = state[h, head + head // 3, KV_ROWS:, :]
                sums.append(jnp.concatenate([key_sum] * (dim_head // (CHUNK - KV_ROWS)), axis=0))
            for s in range(2):
                for i, block in enumerate([parts, sums]):
                    rows = slice((2 * i + s) * dim_head, (2 * i + s + 1) * dim_head)
                    rhs[slot, p, rows, s * half : (s + 1) * half] = block[s]

    operand(0, core)
    for p in range(pairs):
        at = slice(p * 2 * lanes, (p + 1) * 2 * lanes)
        partial[:, at] = dot_t(fq[core, :, at], rhs[0, p])
    wait_received(state.at[1 - core], fw_sem)
    operand(1, 1 - core)
    gain_load.wait()
    o_load.wait()
    for p in range(pairs):
        on = slice(p * 2 * lanes, (p + 1) * 2 * lanes)
        both = partial[:, on] + dot_t(fq[1 - core, :, on], rhs[1, p])
        attn[:, p * lanes : (p + 1) * lanes] = both[:, :lanes] / both[:, lanes:]
    for r in range(rows_here):
        at = slice(r * cols, (r + 1) * cols)
        squares = jnp.zeros((cols, lanes), F32)
        for c in range(0, width, lanes):
            ratio = attn[at, c : c + lanes]
            squares = squares + ratio * ratio
        scale = lax.rsqrt(jnp.sum(squares, axis=1, keepdims=True) * (1.0 / width) + 1e-06)
        for c in range(0, width, lanes):
            normed = attn[at, c : c + lanes] * scale * gain[c : c + lanes].reshape(1, lanes)
            mixed[at, c : c + lanes] = (normed + pos[at, c : c + lanes]).astype(BF16)
        for c in range(0, width, 256):
            out[at, c : c + 256] = (
                tok[at, c : c + 256].astype(F32) + dot(mixed[at], wo[:, c : c + 256])
            ).astype(BF16)
    wait_sent(send0.at[1 - core], pair_sem)
    wait_sent(send1.at[pl.ds(0, NEAR - 1)], rs_sem)
    wait_sent(recv2, far_sem)
    wait_sent(halo, halo_sem)
    wait_sent(state.at[core, pl.ds(0, NEAR - 1)], ag_sem)
    wait_sent(state.at[core], fw_sem)


def layer(n, tokens, w_query, w_key, w_value, w_out, omega, conv_kernel, norm_gain):
    rows_here, cols, width = tokens.shape
    heads, dim_head, nfeat = omega.shape
    count = rows_here * cols
    pairs, lanes, half = heads // 2, 2 * dim_head, nfeat // 2
    far = n // (CORES * NEAR) - 1
    steps = len(STEPS)
    vmem = pltpu.VMEM
    dma = pltpu.SemaphoreType.DMA
    out = pl.pallas_call(
        functools.partial(kernel, n, heads),
        out_shape=jax.ShapeDtypeStruct((count, width), BF16),
        in_specs=[pl.BlockSpec(memory_space=pl.ANY)] * 8,
        out_specs=pl.BlockSpec(memory_space=pltpu.VMEM),
        scratch_shapes=[
            vmem((count, width), BF16),
            vmem((width, width), BF16),
            vmem((width, width), BF16),
            vmem((width, width), BF16),
            vmem((width, width), BF16),
            vmem((heads, dim_head, nfeat), BF16),
            vmem((3, 3, width), F32),
            vmem((width,), F32),
            vmem((pairs, 2, 2 * lanes, nfeat), BF16),
            vmem((count, width), BF16),
            vmem((count + 2 * cols, width), BF16),
            vmem((2, cols, width), BF16),
            vmem((pairs, lanes + 16, count), BF16),
            vmem((2, count, heads * half), BF16),
            vmem((count, width), F32),
            vmem((count, width), F32),
            vmem((count, width), BF16),
            vmem((2, NEAR, CHUNK, half), BF16),
            vmem((NEAR, CHUNK, half), BF16),
            vmem((NEAR, CHUNK, half), BF16),
            vmem((NEAR, CHUNK, half), BF16),
            vmem((CHUNK, half), BF16),
            vmem((far, CHUNK, half), BF16),
            vmem((2, NEAR, CHUNK, half), BF16),
            vmem((2, pairs, 2 * lanes, nfeat), BF16),
            vmem((count, pairs * 2 * lanes), F32),
            dma((8,)),
            dma((1 + WAVES,)),
            dma((2,)),
            dma((2,)),
            dma((2,)),
            dma((1 + ZN,)),
            dma((2,)),
            pltpu.SemaphoreType.REGULAR,
        ],
        compiler_params=pltpu.CompilerParams(
            collective_id=0, has_side_effects=True, vmem_limit_bytes=48 * 1024 * 1024
        ),
        name="favor_layer",
    )(
        *[
            pltpu.with_memory_space_constraint(operand, pltpu.HBM)
            for operand in (
                tokens.reshape(count, width),
                w_query,
                w_key,
                w_value,
                w_out,
                omega,
                conv_kernel,
                norm_gain,
            )
        ]
    )
    return out.reshape(rows_here, cols, width)


def solution(mesh):
    return jax.shard_map(
        functools.partial(layer, mesh.shape["row"]),
        mesh=mesh,
        in_specs=(P(("parts", "row"), None, None), P(), P(), P(), P(), P(), P(), P()),
        out_specs=P(("parts", "row"), None, None),
        check_vma=False,
    )
```
